256 devices in a mesh: cls: 128 (over y, z, x), rep: 2 (over core).
Axes of the slice: x: 4, y: 4, z: 8, core: 2. Of those that a mesh axis runs over, the one named last changes fastest.
Arguments:
- queries: bfloat16 [2, 256, 768], P('rep', 'cls'), may hold values from -16 to 16
- positives: int32 [2, 256, 4], replicated, may hold values from -1 to 786431, as said below
- label_vectors: bfloat16 [786432, 768], P('cls'), may hold values from -80 to 80
- refresh_slot: int32 [], replicated, may hold values from 0 to 7
- features: bfloat16 [98304, 768], P(('cls', 'rep')), may hold values from -6 to 6
- encoder_weight: bfloat16 [768, 768], replicated, may hold values from -0.21875 to 0.21875
- encoder_gain: float32 [768], replicated, may hold values from 0.1 to 1.9
- free_vectors: bfloat16 [98304, 768], P(('cls', 'rep')), may hold values from -3 to 3
- targets: int32 [98304], replicated, may hold values from 0 to 98303, as said below
Outputs:
- loss: float32 [2, 256], P('rep', 'cls')
- query_grads: bfloat16 [2, 256, 768], P('rep', 'cls')
- refreshed_vectors: bfloat16 [98304, 768], P(('cls', 'rep'))
The draws below stay inside these ranges and needn't reach their ends.
Inputs may be any that keep to these rules, and one draw needn't show every extreme that they name: `positives`: each row holds 1 to 4 label ids in its first places and -1 in the rest; ids may repeat within a row. `targets`: A permutation. Refreshed row t belongs to owner t // 768. The b-th aligned block of 384 entries names exactly 3 rows of every owner, all in the half b % 2 of that owner's 768 rows.
All inputs are finite; a program needn't handle non-finite values.
Results may differ from the reference program's by a relative error of at most 0.0048.
Values may be sent and summed in bfloat16 or wider, within the bound.
A program may use at most 128 MiB of HBM per device.

```python
import jax
import jax.numpy as jnp
from jax import lax

D = 768
LAB_DEV = 6144
SLOTS = 8
POS = 4
Q_DEV = 2
LABELS = 786432
R_DEV = 768
REFRESH = 98304
QG = 256
N_CLS = 128
N_REP = 2


def label_rows(key, row_ids):
    row_base = jax.random.fold_in(key, 11)

    def one_row(row_id):
        return jax.random.normal(jax.random.fold_in(row_base, row_id), (D,), jnp.float32)
    values = jnp.clip(jax.vmap(one_row)(row_ids), -6.0, 6.0)
    return values


def draw_label_vectors(key, part):
    return label_rows(key, jnp.arange(LABELS, dtype=jnp.int32)).astype(jnp.bfloat16)


def draw_queries(key, part):
    total_rows = N_REP * Q_DEV * N_CLS
    spread = 3.0 * D ** (-0.5)
    values = spread * jnp.clip(jax.random.normal(jax.random.fold_in(key, 21), (total_rows, D), jnp.float32), -6.0, 6.0)
    return values.reshape(N_REP, Q_DEV * N_CLS, D).astype(jnp.bfloat16)


def draw_positives(key, part):
    total_rows = N_REP * Q_DEV * N_CLS
    counts = jax.random.randint(jax.random.fold_in(key, 31), (total_rows,), 1, POS + 1)
    counts = counts.at[0].set(POS).at[1].set(1)
    label_ids = jax.random.randint(jax.random.fold_in(key, 32), (total_rows, POS), 0, LABELS)
    places = jnp.arange(POS, dtype=jnp.int32)[None, :]
    filled = jnp.where(places < counts[:, None], label_ids, -1)
    return filled.reshape(N_REP, Q_DEV * N_CLS, POS).astype(jnp.int32)


def draw_targets(key, part):
    half_rows = LAB_DEV // SLOTS // N_REP
    per_owner = half_rows // N_CLS
    key_list = jax.random.split(jax.random.fold_in(key, 41), N_REP * N_CLS)
    shuffled = jax.vmap(lambda one_key: jax.random.permutation(one_key, half_rows))(key_list)
    shuffled = shuffled.reshape(N_REP, N_CLS, N_CLS, per_owner)
    owners = jnp.arange(N_CLS, dtype=jnp.int32)[None, :, None, None]
    halves = jnp.arange(N_REP, dtype=jnp.int32)[:, None, None, None]
    rows_all = owners * (half_rows * N_REP) + halves * half_rows + shuffled
    rows_all = rows_all.transpose(2, 0, 1, 3).reshape(N_CLS * N_REP, N_CLS * per_owner)
    order_keys = jax.random.split(jax.random.fold_in(key, 42), N_CLS * N_REP)
    orders = jax.vmap(lambda one_key: jax.random.permutation(one_key, N_CLS * per_owner))(order_keys)
    rows_all = jnp.take_along_axis(rows_all, orders, axis=1)
    return rows_all.reshape(-1).astype(jnp.int32)


def block_levels(key, extent, cuts, low, top_value):
    def one(dim, shards_of):
        heights = jax.random.uniform(jax.random.fold_in(jax.random.fold_in(key, 6), dim), (shards_of,), jnp.float32, low / len(cuts), top_value / len(cuts))
        return jnp.repeat(jnp.exp(heights), extent[dim] // shards_of).reshape((-1,) + (1,) * (len(extent) - dim - 1))

    factor_of = one(*cuts[0])
    for cut in cuts[1:]:
        factor_of = factor_of * one(*cut)
    return factor_of


def normal_values(key, shape, width, limit, cuts=(), held_as=jnp.bfloat16):
    loudness = block_levels(key, shape, cuts, -0.22, 0.18) if cuts else 1.0
    values = jax.random.normal(key, shape, jnp.float32) * width * loudness
    return jnp.minimum(jnp.maximum(values, -limit), limit).astype(held_as)


def setup_inputs(seed: int = 0) -> dict:
    key_of = jax.random.split(jax.random.key(seed), 10)
    return {
        "queries": draw_queries(jax.random.fold_in(key_of[9], 71), 0),
        "positives": draw_positives(jax.random.fold_in(key_of[9], 71), 0),
        "label_vectors": draw_label_vectors(jax.random.fold_in(key_of[9], 71), 0),
        "refresh_slot": jax.random.randint(key_of[3], (), 0, SLOTS).astype(jnp.int32),
        "features": normal_values(key_of[4], (REFRESH, D), 1.0, 6.0, ((0, 256),)),
        "encoder_weight": normal_values(key_of[5], (D, D), D ** -0.5, 0.21875),
        "encoder_gain": jnp.clip(1.0 + 0.18 * jax.random.normal(key_of[6], (D,), jnp.float32), 0.1, 1.9),
        "free_vectors": normal_values(key_of[7], (REFRESH, D), 0.5, 3.0, ((0, 256),)),
        "targets": draw_targets(jax.random.fold_in(key_of[9], 71), 0),
    }


def reference(queries, positives, label_vectors, refresh_slot, features, encoder_weight, encoder_gain, free_vectors, targets):
    hidden = jnp.dot(features, encoder_weight, preferred_element_type=jnp.float32)
    normed = hidden * lax.rsqrt(lax.optimization_barrier(jnp.mean(hidden * hidden, axis=1, keepdims=True)) + 1e-06) * encoder_gain
    encoded = lax.optimization_barrier(normed.astype(jnp.bfloat16))
    placed = jnp.zeros((REFRESH, D), jnp.bfloat16).at[targets].set(encoded)
    refreshed = (free_vectors.astype(jnp.float32) + placed.astype(jnp.float32)).astype(jnp.bfloat16)
    blocks = label_vectors.reshape(N_CLS, SLOTS, R_DEV, D)
    zero_index = jnp.zeros((), jnp.int32)
    current = lax.dynamic_update_slice(blocks, refreshed.reshape(N_CLS, 1, R_DEV, D), (zero_index, refresh_slot.astype(jnp.int32), zero_index, zero_index)).reshape(LABELS, D)
    block_size = Q_DEV * 32
    query_blocks = queries.reshape(-1, block_size, D)
    positive_blocks = positives.reshape(-1, block_size, POS)

    def one_block(block_pair):
        block_queries, block_ids = block_pair
        logits = lax.dot_general(block_queries, current, (((1,), (1,)), ((), ())), preferred_element_type=jnp.float32)
        maximum = lax.optimization_barrier(jnp.max(logits, axis=1))
        exp_total = lax.optimization_barrier(jnp.sum(jnp.exp(logits - maximum[:, None]), axis=1))
        log_total = maximum + jnp.log(exp_total)
        valid_ids = block_ids >= 0
        safe_ids = jnp.where(valid_ids, block_ids, 0).astype(jnp.int32)
        picked = jnp.take_along_axis(logits, safe_ids, axis=1)
        id_count = lax.optimization_barrier(jnp.sum(valid_ids.astype(jnp.float32), axis=1))
        positive_sum = lax.optimization_barrier(jnp.sum(jnp.where(valid_ids, picked, jnp.zeros_like(picked)), axis=1))
        block_loss = log_total - positive_sum / id_count
        id_weight = jnp.where(valid_ids, jnp.ones_like(picked), jnp.zeros_like(picked)) / id_count[:, None]
        row_index = jnp.broadcast_to(jnp.arange(block_ids.shape[0], dtype=jnp.int32)[:, None], block_ids.shape)
        target_mass = jnp.zeros(logits.shape, jnp.float32).at[row_index, safe_ids].add(id_weight)
        coefficients = (jnp.exp(logits - log_total[:, None]) - target_mass).astype(jnp.bfloat16)
        block_grads = jnp.dot(coefficients, current, preferred_element_type=jnp.float32).astype(jnp.bfloat16)
        return (block_loss, block_grads)
    losses, grads = lax.map(one_block, (query_blocks, positive_blocks))
    return (losses.reshape(N_REP, QG), grads.reshape(N_REP, QG, D), refreshed)
```

```python
import jax
import jax.numpy as jnp
from jax import lax
from jax.experimental import pallas as pl
from jax.experimental.pallas import tpu as pltpu
from jax.sharding import Mesh
from jax.sharding import PartitionSpec as P

F32 = jnp.float32
BF16 = jnp.bfloat16
I32 = jnp.int32
MESH = pl.DeviceIdType.MESH
CLS = ("y", "z", "x")
CLS_REP = ("y", "z", "x", "core")
NY, NZ, NX = 4, 8, 4
NPLANE = NX * NY
NCLS = NPLANE * NZ
D = 768
HALF = D // 2
ROWS = 384
SLOTS = 8
SLOT_ROWS = 768
LABELS_DEV = SLOTS * SLOT_ROWS
NQ = 256
POS = 4
CHUNK = 32
LANES = 128
TILES = SLOT_ROWS // LANES


def dot(a, b):
    return jnp.dot(a, b, preferred_element_type=F32)


def dot_t(a, b):
    return lax.dot_general(a, b, (((1,), (1,)), ((), ())), preferred_element_type=F32)


def each(lo, hi, fn):
    def step(k, carry):
        fn(k)
        return carry

    lax.fori_loop(lo, hi, step, 0)


def three_of(parts, inside):
    low = high = total = None
    for part, mask in zip(parts, inside):
        lo = jnp.min(jnp.where(mask, part, 1e9), axis=1, keepdims=True)
        hi = jnp.max(jnp.where(mask, part, -1.0), axis=1, keepdims=True)
        su = jnp.sum(jnp.where(mask, part, 0.0), axis=1, keepdims=True)
        low = lo if low is None else jnp.minimum(low, lo)
        high = hi if high is None else jnp.maximum(high, hi)
        total = su if total is None else total + su
    return low, total - low - high, high


def merged(stats, count):
    peak = stats[0, 0:1, :]
    for i in range(1, count):
        peak = jnp.maximum(peak, stats[i, 0:1, :])
    total = jnp.zeros_like(peak)
    positive = jnp.zeros_like(peak)
    for i in range(count):
        total = total + stats[i, 1:2, :] * jnp.exp(stats[i, 0:1, :] - peak)
        positive = positive + stats[i, 2:3, :]
    return peak, total, positive


def kernel(
    slot_ref, q_hbm, pos_ref, lab_hbm, feat_ref, w_ref, gain_ref, free_hbm, tgt_ref,
    loss_ref, grad_ref, fresh_hbm,
    qg, qm, lab, free, enc2, send, recv, fresh, off, inv, lg, tm, mx, sacc, pacc, ltb, coef, gacc,
    gsend, grecv, hsend, hrecv, st_p, st_z,
    ready,
    lab_sem, free_sem, q_sem, out_sem,
    qz_s, qz_r, qp_s, qp_r, d_s, d_r, f_s, f_r, sp_s, sp_r, sz_s, sz_r, gp_s, gp_r, gz_s, gz_r,
):
    y, z, x = lax.axis_index("y"), lax.axis_index("z"), lax.axis_index("x")
    core = lax.axis_index("core")
    me = (y * NZ + z) * NX + x
    plane = x * NY + y

    def z_peer(k):
        return (z + k) % NZ

    def plane_peer(k):
        return (x + k // NY) % NX, (y + k % NY) % NY

    def wait_all(ref, s, r):
        pltpu.make_async_copy(ref, ref, r).wait()
        pltpu.make_async_copy(ref, ref, s).wait()

    barrier = pltpu.get_barrier_semaphore()

    def greet_z(k):
        pl.semaphore_signal(barrier, inc=1, device_id={"z": z_peer(k)}, device_id_type=MESH)

    def greet_plane(k):
        tx, ty = plane_peer(k)
        pl.semaphore_signal(barrier, inc=1, device_id={"x": tx, "y": ty}, device_id_type=MESH)

    each(1, NZ, greet_z)
    each(1, NPLANE, greet_plane)
    pl.semaphore_signal(barrier, inc=1, device_id={"core": 1 - core}, device_id_type=MESH)

    q_copy = pltpu.make_async_copy(q_hbm, qg.at[plane, z], q_sem)
    q_copy.start()
    lab_copy = pltpu.make_async_copy(lab_hbm, lab, lab_sem)
    lab_copy.start()
    free_copy = pltpu.make_async_copy(free_hbm, free, free_sem)
    free_copy.start()

    hidden = dot(feat_ref[...], w_ref[...])
    scale = lax.rsqrt(jnp.mean(hidden * hidden, axis=1, keepdims=True) + 1e-06)
    encoded = (hidden * scale * gain_ref[...]).astype(BF16)
    enc2[0:ROWS, :] = encoded[:, 0:HALF]
    enc2[ROWS : 2 * ROWS, :] = encoded[:, HALF:D]

    q_copy.wait()
    pl.semaphore_wait(barrier, NZ - 1 + NPLANE - 1 + 1)

    def ready_z(k):
        pl.semaphore_signal(ready, inc=1, device_id={"z": z_peer(k)}, device_id_type=MESH)

    def gather_z(k):
        pltpu.make_async_remote_copy(
            qg.at[plane, z], qg.at[plane, z], qz_s, qz_r, device_id={"z": z_peer(k)}, device_id_type=MESH
        ).start()

    each(1, NZ, ready_z)
    each(1, NZ, gather_z)

    block = me * 2 + core
    row = lax.broadcasted_iota(I32, (2 * NCLS, LANES), 0)
    owner_base = (row // 2) * SLOT_ROWS
    parts = []
    inside = []
    for k in range(3):
        part = tgt_ref[pl.ds(3 * block + k, 1), :] - owner_base
        parts.append(part.astype(F32))
        inside.append((part >= 0) & (part < SLOT_ROWS))
    picks = three_of(parts, inside)
    even = row % 2 == 0
    for r in range(3):
        hit = [part == picks[r] for part in parts]
        one = [jnp.where(h & even, 1.0, 0.0).astype(BF16) for h in hit]
        two = [jnp.where(h & ~even, 1.0, 0.0).astype(BF16) for h in hit]
        chosen = dot(jnp.concatenate(one + two, axis=1), enc2[...])
        send[:, :, r * HALF : (r + 1) * HALF] = chosen.astype(BF16).reshape(NCLS, 2, HALF)

    wait_all(qg.at[plane, pl.ds(0, NZ - 1)], qz_s, qz_r)
    pl.semaphore_wait(ready, NZ - 1)

    def gather_plane(k):
        tx, ty = plane_peer(k)
        pltpu.make_async_remote_copy(
            qg.at[plane], qg.at[plane], qp_s, qp_r, device_id={"x": tx, "y": ty}, device_id_type=MESH
        ).start()

    def dispatch(k):
        tz = z_peer(k % NZ)
        tx, ty = plane_peer(k // NZ)
        dest = (ty * NZ + tz) * NX + tx
        pltpu.make_async_remote_copy(
            send.at[dest], recv.at[me], d_s, d_r, device_id={"y": ty, "z": tz, "x": tx}, device_id_type=MESH
        ).start()

    each(1, NPLANE, gather_plane)
    each(1, NCLS, dispatch)
    recv[me] = send[me]

    parts = []
    inside = []
    for k in range(3):
        first = tgt_ref[pl.ds(k, NCLS, stride=6), :]
        second = tgt_ref[pl.ds(3 + k, NCLS, stride=6), :]
        part = jnp.where(core == 0, first, second) - (me * SLOT_ROWS + core * ROWS)
        parts.append(part.astype(F32))
        inside.append((part >= 0) & (part < ROWS))
    picks = three_of(parts, inside)
    lane = lax.broadcasted_iota(I32, (NCLS, ROWS), 1).astype(F32)
    put = jnp.concatenate([jnp.where(lane == p, 1.0, 0.0).astype(BF16) for p in picks], axis=0)

    slot = slot_ref[0]
    ids = pos_ref[core]
    valid = ids >= 0
    count = jnp.sum(jnp.where(valid, 1.0, 0.0), axis=1, keepdims=True)
    inv[...] = jnp.broadcast_to(1.0 / count, (NQ, LANES))
    local = jnp.where(valid, ids - me * LABELS_DEV, -LABELS_DEV)
    for j in range(POS):
        off[j] = jnp.broadcast_to(local[:, j : j + 1], (NQ, LANES))

    def slot_of(k):
        return lax.rem(slot + 1 + k, SLOTS)

    nblocks = NQ // CHUNK

    def mass(k):
        base = slot_of(k) * SLOT_ROWS

        def rows(b):
            at = pl.ds(b * CHUNK, CHUNK)
            share = inv[at, :]
            lane_id = lax.broadcasted_iota(I32, (CHUNK, LANES), 1) + base
            offs = [off[j, at, :] - lane_id for j in range(POS)]
            for c in range(TILES):
                acc = jnp.zeros((CHUNK, LANES), F32)
                for j in range(POS):
                    acc = acc + jnp.where(offs[j] == c * LANES, share, 0.0)
                tm[k, at, c * LANES : (c + 1) * LANES] = acc

        each(0, nblocks, rows)

    each(0, SLOTS, mass)

    lab_copy.wait()
    wait_all(qg.at[pl.ds(0, NPLANE - 1)], qp_s, qp_r)
    qm[...] = qg[...].reshape(NQ, D)

    def peaks(k, values):
        lg[k] = values
        top = values[:, 0:LANES]
        for c in range(1, TILES):
            top = jnp.maximum(top, values[:, c * LANES : (c + 1) * LANES])
        return top

    def logits_of(k, peak):
        return jnp.maximum(peak, peaks(k, dot_t(qm[...], lab[slot_of(k)])))

    peak = lax.fori_loop(0, SLOTS - 1, logits_of, jnp.full((NQ, LANES), -jnp.inf, F32))
    mx[...] = jnp.broadcast_to(jnp.max(peak, axis=1, keepdims=True), (NQ, LANES))
    sacc[...] = jnp.zeros((NQ, LANES), F32)
    pacc[...] = jnp.zeros((NQ, LANES), F32)

    def sums(k):
        def rows(b):
            at = pl.ds(b * CHUNK, CHUNK)
            top = mx[at, :]
            s = sacc[at, :]
            p = pacc[at, :]
            for c in range(TILES):
                value = lg[k, at, c * LANES : (c + 1) * LANES]
                s = s + jnp.exp(value - top)
                p = p + tm[k, at, c * LANES : (c + 1) * LANES] * value
            sacc[at, :] = s
            pacc[at, :] = p

        each(0, nblocks, rows)

    each(0, SLOTS - 1, sums)

    free_copy.wait()
    wait_all(recv.at[pl.ds(0, NCLS - 1)], d_s, d_r)
    arrived = recv[...].reshape(2 * NCLS, 3 * HALF)
    pick_row = lax.broadcasted_iota(I32, (NCLS, 2 * NCLS), 0) * 2
    pick_col = lax.broadcasted_iota(I32, (NCLS, 2 * NCLS), 1)
    for c in range(2):
        take = jnp.where(pick_col == pick_row + c, 1.0, 0.0).astype(BF16)
        half = dot(take, arrived).astype(BF16)
        stacked = jnp.concatenate([half[:, r * HALF : (r + 1) * HALF] for r in range(3)], axis=0)
        placed = lax.dot_general(put, stacked, (((0,), (0,)), ((), ())), preferred_element_type=F32)
        cols = slice(c * HALF, (c + 1) * HALF)
        fresh[core, :, cols] = (free[:, cols].astype(F32) + placed).astype(BF16)
    swap = pltpu.make_async_remote_copy(
        fresh.at[core], fresh.at[core], f_s, f_r, device_id={"core": 1 - core}, device_id_type=MESH
    )
    swap.start()
    out_copy = pltpu.make_async_copy(fresh.at[core], fresh_hbm, out_sem)
    out_copy.start()
    swap.wait()
    new = fresh[...].reshape(SLOT_ROWS, D)
    peak = peaks(SLOTS - 1, dot_t(qm[...], new))
    old = mx[...]
    top = jnp.maximum(old, jnp.broadcast_to(jnp.max(peak, axis=1, keepdims=True), (NQ, LANES)))
    sacc[...] = sacc[...] * jnp.exp(old - top)
    mx[...] = top
    sums(SLOTS - 1)

    st_p[plane, 0:1, :] = mx[...].T[0:1, :]
    st_p[plane, 1:2, :] = jnp.sum(sacc[...].T, axis=0, keepdims=True)
    st_p[plane, 2:3, :] = jnp.sum(pacc[...].T, axis=0, keepdims=True)
    st_p[plane, 3:4, :] = jnp.zeros((1, NQ), F32)

    def stats_plane(k):
        tx, ty = plane_peer(k)
        pltpu.make_async_remote_copy(
            st_p.at[plane], st_p.at[plane], sp_s, sp_r, device_id={"x": tx, "y": ty}, device_id_type=MESH
        ).start()

    each(1, NPLANE, stats_plane)
    wait_all(st_p.at[pl.ds(0, NPLANE - 1)], sp_s, sp_r)
    peak, total, positive = merged(st_p, NPLANE)
    st_z[z, 0:1, :] = peak
    st_z[z, 1:2, :] = total
    st_z[z, 2:3, :] = positive
    st_z[z, 3:4, :] = jnp.zeros((1, NQ), F32)

    def stats_z(k):
        pltpu.make_async_remote_copy(
            st_z.at[z], st_z.at[z], sz_s, sz_r, device_id={"z": z_peer(k)}, device_id_type=MESH
        ).start()

    each(1, NZ, stats_z)
    wait_all(st_z.at[pl.ds(0, NZ - 1)], sz_s, sz_r)
    peak, total, positive = merged(st_z, NZ)
    log_total = peak + jnp.log(total)
    loss = log_total - positive
    own = (plane * NZ + z) * 2
    query = lax.broadcasted_iota(I32, (1, NQ), 1)
    for i in range(2):
        loss_ref[:, i : i + 1] = jnp.sum(jnp.where(query == own + i, loss, 0.0), axis=1, keepdims=True)
    ltb[...] = jnp.broadcast_to(log_total, (LANES, NQ)).T

    def coefficients(k):
        def rows(b):
            at = pl.ds(b * CHUNK, CHUNK)
            level = ltb[at, :]
            for c in range(TILES):
                cols = slice(c * LANES, (c + 1) * LANES)
                coef[k, at, cols] = (jnp.exp(lg[k, at, cols] - level) - tm[k, at, cols]).astype(BF16)

        each(0, nblocks, rows)

    each(0, SLOTS, coefficients)
    gacc[...] = dot(coef[SLOTS - 1], new)

    def gradients(k):
        gacc[...] += dot(coef[k], lab[slot_of(k)])

    each(0, SLOTS - 1, gradients)
    gsend[...] = gacc[...].astype(BF16).reshape(NPLANE, 2 * NZ, D)

    def scatter_plane(k):
        tx, ty = plane_peer(k)
        pltpu.make_async_remote_copy(
            gsend.at[tx * NY + ty], grecv.at[plane], gp_s, gp_r, device_id={"x": tx, "y": ty}, device_id_type=MESH
        ).start()

    each(1, NPLANE, scatter_plane)
    grecv[plane] = gsend[plane]
    wait_all(grecv.at[pl.ds(0, NPLANE - 1)], gp_s, gp_r)
    part = grecv[0].astype(F32)
    for i in range(1, NPLANE):
        part = part + grecv[i].astype(F32)
    hsend[...] = part.reshape(NZ, 2, D)

    def scatter_z(k):
        tz = z_peer(k)
        pltpu.make_async_remote_copy(
            hsend.at[tz], hrecv.at[z], gz_s, gz_r, device_id={"z": tz}, device_id_type=MESH
        ).start()

    each(1, NZ, scatter_z)
    hrecv[z] = hsend[z]
    wait_all(hrecv.at[pl.ds(0, NZ - 1)], gz_s, gz_r)
    whole = hrecv[0]
    for i in range(1, NZ):
        whole = whole + hrecv[i]
    grad_ref[...] = whole.astype(BF16)
    out_copy.wait()


def per_device(
    queries,
    positives,
    label_vectors,
    refresh_slot,
    features,
    encoder_weight,
    encoder_gain,
    free_vectors,
    targets,
):
    in_order = positives.reshape(2, NY, NZ, NX, 2, POS).transpose(0, 3, 1, 2, 4, 5).reshape(2, NQ, POS)
    vmem = pl.BlockSpec(memory_space=pltpu.VMEM)
    hbm = pl.BlockSpec(memory_space=pl.ANY)
    dma = pltpu.SemaphoreType.DMA
    loss, grads, refreshed = pl.pallas_call(
        kernel,
        out_shape=(
            jax.ShapeDtypeStruct((1, 2), F32),
            jax.ShapeDtypeStruct((2, D), BF16),
            jax.ShapeDtypeStruct((ROWS, D), BF16),
        ),
        in_specs=[pl.BlockSpec(memory_space=pltpu.SMEM), hbm, vmem, hbm, vmem, vmem, vmem, hbm, vmem],
        out_specs=(vmem, vmem, hbm),
        scratch_shapes=[
            pltpu.VMEM((NPLANE, NZ, 2, D), BF16),
            pltpu.VMEM((NQ, D), BF16),
            pltpu.VMEM((SLOTS, SLOT_ROWS, D), BF16),
            pltpu.VMEM((ROWS, D), BF16),
            pltpu.VMEM((2 * ROWS, HALF), BF16),
            pltpu.VMEM((NCLS, 2, 3 * HALF), BF16),
            pltpu.VMEM((NCLS, 2, 3 * HALF), BF16),
            pltpu.VMEM((2, ROWS, D), BF16),
            pltpu.VMEM((POS, NQ, LANES), I32),
            pltpu.VMEM((NQ, LANES), F32),
            pltpu.VMEM((SLOTS, NQ, SLOT_ROWS), F32),
            pltpu.VMEM((SLOTS, NQ, SLOT_ROWS), F32),
            pltpu.VMEM((NQ, LANES), F32),
            pltpu.VMEM((NQ, LANES), F32),
            pltpu.VMEM((NQ, LANES), F32),
            pltpu.VMEM((NQ, LANES), F32),
            pltpu.VMEM((SLOTS, NQ, SLOT_ROWS), BF16),
            pltpu.VMEM((NQ, D), F32),
            pltpu.VMEM((NPLANE, 2 * NZ, D), BF16),
            pltpu.VMEM((NPLANE, 2 * NZ, D), BF16),
            pltpu.VMEM((NZ, 2, D), F32),
            pltpu.VMEM((NZ, 2, D), F32),
            pltpu.VMEM((NPLANE, 4, NQ), F32),
            pltpu.VMEM((NZ, 4, NQ), F32),
            pltpu.SemaphoreType.REGULAR,
        ]
        + [dma] * 20,
        compiler_params=pltpu.CompilerParams(
            collective_id=0, has_side_effects=True, vmem_limit_bytes=60 * 2**20
        ),
    )(
        refresh_slot.reshape(1),
        queries.reshape(2, D),
        in_order,
        label_vectors.reshape(SLOTS, SLOT_ROWS, D),
        features,
        encoder_weight,
        encoder_gain.reshape(1, D),
        free_vectors,
        targets.reshape(-1, LANES),
    )
    return loss, grads.reshape(1, 2, D), refreshed


def solution(mesh):
    torus = Mesh(mesh.devices.reshape(NY, NZ, NX, mesh.shape["rep"]), CLS_REP)
    placed = (
        P("core", CLS, None),
        P(),
        P(CLS, None),
        P(),
        P(CLS_REP, None),
        P(),
        P(),
        P(CLS_REP, None),
        P(),
    )
    return jax.shard_map(
        per_device,
        mesh=torus,
        in_specs=placed,
        out_specs=(P("core", CLS), P("core", CLS, None), P(CLS_REP, None)),
        check_vma=False,
    )
```

```python
import jax
import jax.numpy as jnp
from jax import lax
from jax.experimental import pallas as pl
from jax.experimental.pallas import tpu as pltpu
from jax.sharding import Mesh
from jax.sharding import PartitionSpec as P

F32 = jnp.float32
BF16 = jnp.bfloat16
I32 = jnp.int32
MESH = pl.DeviceIdType.MESH
CLS = ("y", "z", "x")
CLS_REP = ("y", "z", "x", "core")
NY, NZ, NX = 4, 8, 4
NPLANE = NX * NY
NCLS = NPLANE * NZ
D = 768
HALF = D // 2
ROWS = 384
SLOTS = 8
SLOT_ROWS = 768
LABELS_DEV = SLOTS * SLOT_ROWS
NQ = 256
POS = 4
CHUNK = 32
LANES = 128
TILES = SLOT_ROWS // LANES
EARLY = 3
MIDDLE = 5


def dot(a, b):
    return jnp.dot(a, b, preferred_element_type=F32)


def dot_t(a, b):
    return lax.dot_general(a, b, (((1,), (1,)), ((), ())), preferred_element_type=F32)


def each(lo, hi, fn):
    def step(k, carry):
        fn(k)
        return carry

    lax.fori_loop(lo, hi, step, 0)


def three_of(parts, inside):
    low = high = total = None
    for part, mask in zip(parts, inside):
        lo = jnp.min(jnp.where(mask, part, 1e9), axis=1, keepdims=True)
        hi = jnp.max(jnp.where(mask, part, -1.0), axis=1, keepdims=True)
        su = jnp.sum(jnp.where(mask, part, 0.0), axis=1, keepdims=True)
        low = lo if low is None else jnp.minimum(low, lo)
        high = hi if high is None else jnp.maximum(high, hi)
        total = su if total is None else total + su
    return low, total - low - high, high


def merged(stats, count):
    peak = stats[0, 0:1, :]
    for i in range(1, count):
        peak = jnp.maximum(peak, stats[i, 0:1, :])
    total = jnp.zeros_like(peak)
    positive = jnp.zeros_like(peak)
    for i in range(count):
        total = total + stats[i, 1:2, :] * jnp.exp(stats[i, 0:1, :] - peak)
        positive = positive + stats[i, 2:3, :]
    return peak, total, positive


def kernel(
    slot_ref, q_hbm, pos_hbm, lab_hbm, feat_hbm, w_hbm, gain_hbm, free_hbm, tgt_hbm,
    loss_ref, grad_ref, fresh_hbm,
    pos_ref, feat_ref, w_ref, gain_ref, tgt_ref,
    qg, qm, lab, free, enc2, send, recv, put, fresh, off, inv, lg, cnt, mx, top_ref, sacc, pacc, ltb, coef, gacc, gu, gt,
    gsend, grecv, hsend, hrecv, st_p, st_z,
    ready,
    lab_sem, free_sem, q_sem, out_sem, w_sem, feat_sem, small_sem,
    qz_s, qz_r, qp_s, qp_r, d_s, d_r, f_s, f_r, sp_s, sp_r, sz_s, sz_r, gp_s, gp_r, gz_s, gz_r,
):
    y, z, x = lax.axis_index("y"), lax.axis_index("z"), lax.axis_index("x")
    core = lax.axis_index("core")
    me = (y * NZ + z) * NX + x
    plane = x * NY + y

    def z_peer(k):
        return (z + k) % NZ

    def plane_peer(k):
        return (x + k // NY) % NX, (y + k % NY) % NY

    def wait_all(ref, s, r):
        pltpu.make_async_copy(ref, ref, r).wait()
        pltpu.make_async_copy(ref, ref, s).wait()

    barrier = pltpu.get_barrier_semaphore()

    def greet_z(k):
        pl.semaphore_signal(barrier, inc=1, device_id={"z": z_peer(k)}, device_id_type=MESH)

    def greet_plane(k):
        tx, ty = plane_peer(k)
        pl.semaphore_signal(barrier, inc=1, device_id={"x": tx, "y": ty}, device_id_type=MESH)

    each(1, NZ, greet_z)
    each(1, NPLANE, greet_plane)
    pl.semaphore_signal(barrier, inc=1, device_id={"core": 1 - core}, device_id_type=MESH)

    q_copy = pltpu.make_async_copy(q_hbm, qg.at[plane, z], q_sem)
    w_copy = pltpu.make_async_copy(w_hbm, w_ref, w_sem)
    feat_copy = pltpu.make_async_copy(feat_hbm, feat_ref, feat_sem)
    gain_copy = pltpu.make_async_copy(gain_hbm, gain_ref, small_sem.at[0])
    pos_copy = pltpu.make_async_copy(pos_hbm, pos_ref, small_sem.at[1])
    tgt_copy = pltpu.make_async_copy(tgt_hbm, tgt_ref, small_sem.at[2])
    free_copy = pltpu.make_async_copy(free_hbm, free, free_sem)
    lab_copy = pltpu.make_async_copy(lab_hbm, lab, lab_sem)
    for copy in (w_copy, feat_copy, q_copy, gain_copy, tgt_copy, pos_copy, free_copy, lab_copy):
        copy.start()

    w_copy.wait()
    feat_copy.wait()
    gain_copy.wait()
    hidden = dot(feat_ref[...], w_ref[...])
    scale = lax.rsqrt(jnp.mean(hidden * hidden, axis=1, keepdims=True) + 1e-06)
    for c in range(2):
        for j in range(TILES // 2):
            i = c * (TILES // 2) + j
            cols = hidden[:, i * LANES : (i + 1) * LANES] * scale * gain_ref[i : i + 1, :]
            enc2[c * ROWS : (c + 1) * ROWS, j * LANES : (j + 1) * LANES] = cols.astype(BF16)

    q_copy.wait()
    pl.semaphore_wait(barrier, NZ - 1 + NPLANE - 1 + 1)

    def ready_z(k):
        pl.semaphore_signal(ready, inc=1, device_id={"z": z_peer(k)}, device_id_type=MESH)

    def gather_z(k):
        pltpu.make_async_remote_copy(
            qg.at[plane, z], qg.at[plane, z], qz_s, qz_r, device_id={"z": z_peer(k)}, device_id_type=MESH
        ).start()

    each(1, NZ, ready_z)
    each(1, NZ, gather_z)

    tgt_copy.wait()
    block = me * 2 + core
    row = lax.broadcasted_iota(I32, (2 * NCLS, LANES), 0)
    owner_base = (row // 2) * SLOT_ROWS
    parts = []
    inside = []
    for k in range(3):
        part = tgt_ref[pl.ds(3 * block + k, 1), :] - owner_base
        parts.append(part.astype(F32))
        inside.append((part >= 0) & (part < SLOT_ROWS))
    picks = three_of(parts, inside)
    even = row % 2 == 0
    for r in range(3):
        hit = [part == picks[r] for part in parts]
        one = [jnp.where(h & even, 1.0, 0.0).astype(BF16) for h in hit]
        two = [jnp.where(h & ~even, 1.0, 0.0).astype(BF16) for h in hit]
        chosen = dot(jnp.concatenate(one + two, axis=1), enc2[...])
        send[:, :, r * HALF : (r + 1) * HALF] = chosen.astype(BF16).reshape(NCLS, 2, HALF)

    wait_all(qg.at[plane, pl.ds(0, NZ - 1)], qz_s, qz_r)
    pl.semaphore_wait(ready, NZ - 1)

    def gather_plane(k):
        tx, ty = plane_peer(k)
        pltpu.make_async_remote_copy(
            qg.at[plane], qg.at[plane], qp_s, qp_r, device_id={"x": tx, "y": ty}, device_id_type=MESH
        ).start()

    def dispatch(k):
        tz = z_peer(k % NZ)
        tx, ty = plane_peer(k // NZ)
        dest = (ty * NZ + tz) * NX + tx
        pltpu.make_async_remote_copy(
            send.at[dest], recv.at[me], d_s, d_r, device_id={"y": ty, "z": tz, "x": tx}, device_id_type=MESH
        ).start()

    each(1, NPLANE, gather_plane)
    each(1, NCLS, dispatch)
    recv[me] = send[me]

    parts = []
    inside = []
    for k in range(3):
        first = tgt_ref[pl.ds(k, NCLS, stride=6), :]
        second = tgt_ref[pl.ds(3 + k, NCLS, stride=6), :]
        part = jnp.where(core == 0, first, second) - (me * SLOT_ROWS + core * ROWS)
        parts.append(part.astype(F32))
        inside.append((part >= 0) & (part < ROWS))
    picks = three_of(parts, inside)
    lane = lax.broadcasted_iota(I32, (NCLS, ROWS), 1).astype(F32)
    spread_row = lax.broadcasted_iota(I32, (NCLS, 2 * NCLS), 0) * 2
    spread_col = lax.broadcasted_iota(I32, (NCLS, 2 * NCLS), 1)
    for r in range(3):
        to_row = jnp.where(lane == picks[r], 1.0, 0.0).T.astype(BF16)
        for c in range(2):
            spread = jnp.where(spread_col == spread_row + c, 1.0, 0.0).astype(BF16)
            put[c, :, r * 2 * NCLS : (r + 1) * 2 * NCLS] = dot(to_row, spread).astype(BF16)

    pos_copy.wait()
    slot = slot_ref[0]
    q_row = lax.broadcasted_iota(I32, (NQ, NQ), 0)
    q_col = lax.broadcasted_iota(I32, (NQ, NQ), 1)
    natural = ((((q_row // 16) % NY) * NZ + (q_row // 2) % NZ) * NX + q_row // 64) * 2 + q_row % 2
    order = jnp.where(q_col == natural, 1.0, 0.0).astype(BF16)
    ids = pos_ref[core] + 1
    ids = sum(
        dot_t(order, ((ids >> (8 * i)) & 255).astype(F32).astype(BF16)) * float(256**i) for i in range(3)
    )
    valid = ids >= 1.0
    count = jnp.sum(jnp.where(valid, 1.0, 0.0), axis=1, keepdims=True)
    inv[...] = jnp.broadcast_to(1.0 / count, (NQ, LANES))
    local = jnp.where(valid, ids.astype(I32) - (1 + me * LABELS_DEV), -LABELS_DEV)
    for j in range(POS):
        off[j] = jnp.broadcast_to(local[:, j : j + 1], (NQ, LANES))

    def slot_of(k):
        return lax.rem(slot + 1 + k, SLOTS)

    nblocks = NQ // CHUNK

    def counts(k):
        base = slot_of(k) * SLOT_ROWS

        def rows(b):
            at = pl.ds(b * CHUNK, CHUNK)
            lane_id = lax.broadcasted_iota(I32, (CHUNK, LANES), 1) + base
            offs = [off[j, at, :] - lane_id for j in range(POS)]
            for c in range(TILES):
                acc = jnp.zeros((CHUNK, LANES), F32)
                for j in range(POS):
                    acc = acc + jnp.where(offs[j] == c * LANES, 1.0, 0.0)
                cnt[k, at, c * LANES : (c + 1) * LANES] = acc.astype(BF16)

        each(0, nblocks, rows)

    each(0, SLOTS, counts)

    lab_copy.wait()
    wait_all(qg.at[pl.ds(0, NPLANE - 1)], qp_s, qp_r)
    qm[...] = qg[...].reshape(NQ, D)

    def highest(values):
        top = values[:, 0:LANES]
        for c in range(1, values.shape[1] // LANES):
            top = jnp.maximum(top, values[:, c * LANES : (c + 1) * LANES])
        return top

    def logits_of(k, peak):
        values = dot_t(qm[...], lab[slot_of(k)])
        lg[k] = values
        return jnp.maximum(peak, highest(values))

    peak = lax.fori_loop(0, SLOTS - 1, logits_of, jnp.full((NQ, LANES), -jnp.inf, F32))
    mx[...] = jnp.broadcast_to(jnp.max(peak, axis=1, keepdims=True), (NQ, LANES))
    sacc[...] = jnp.zeros((NQ, LANES), F32)
    pacc[...] = jnp.zeros((NQ, LANES), F32)

    def weights(k, level_ref):
        def rows(b):
            at = pl.ds(b * CHUNK, CHUNK)
            low_at = pl.ds(NQ + b * CHUNK, CHUNK)
            level = level_ref[at, :]
            s = sacc[at, :]
            p = pacc[at, :]
            for c in range(TILES):
                cols = slice(c * LANES, (c + 1) * LANES)
                value = lg[k, at, cols]
                many = cnt[k, at, cols].astype(F32)
                e = jnp.exp(value - level)
                s = s + e
                p = p + many * value
                high = e.astype(BF16)
                coef[k, at, cols] = high
                coef[k, low_at, cols] = jnp.where(many > 0.0, e - high.astype(F32), 0.0).astype(BF16)
            sacc[at, :] = s
            pacc[at, :] = p

        each(0, nblocks, rows)

    each(0, SLOTS - 1, lambda k: weights(k, mx))
    gacc[...] = jnp.zeros((3 * NQ, D), F32)

    def gradients(k):
        vectors = lab[slot_of(k)]
        gacc[0 : 2 * NQ, :] += dot(coef[k], vectors)
        gacc[2 * NQ : 3 * NQ, :] += dot(cnt[k], vectors)

    each(0, EARLY, gradients)

    free_copy.wait()
    wait_all(recv.at[pl.ds(0, NCLS - 1)], d_s, d_r)
    arrived = recv[...].reshape(2 * NCLS, 3 * HALF)
    stacked = jnp.concatenate([arrived[:, r * HALF : (r + 1) * HALF] for r in range(3)], axis=0)
    swaps = []
    for h in range(2):
        at = slice(h * (ROWS // 2), (h + 1) * (ROWS // 2))
        for c in range(2):
            cols = slice(c * HALF, (c + 1) * HALF)
            fresh[core, at, cols] = (free[at, cols].astype(F32) + dot(put[c, at, :], stacked)).astype(BF16)
        swap = pltpu.make_async_remote_copy(
            fresh.at[core, at], fresh.at[core, at], f_s.at[h], f_r.at[h],
            device_id={"core": 1 - core}, device_id_type=MESH,
        )
        swap.start()
        swaps.append(swap)
    out_copy = pltpu.make_async_copy(fresh.at[core], fresh_hbm, out_sem)
    out_copy.start()
    own_logits = dot_t(qm[...], fresh[core])
    for swap in swaps:
        swap.wait()
    other_logits = dot_t(qm[...], fresh[1 - core])
    peak = jnp.maximum(highest(own_logits), highest(other_logits))
    lg[SLOTS - 1, :, 0:ROWS] = jnp.where(core == 0, own_logits, other_logits)
    lg[SLOTS - 1, :, ROWS : 2 * ROWS] = jnp.where(core == 0, other_logits, own_logits)
    old = mx[...]
    top = jnp.maximum(old, jnp.broadcast_to(jnp.max(peak, axis=1, keepdims=True), (NQ, LANES)))
    sacc[...] = sacc[...] * jnp.exp(old - top)
    top_ref[...] = top
    weights(SLOTS - 1, top_ref)

    st_p[plane, 0:1, :] = top_ref[...].T[0:1, :]
    st_p[plane, 1:2, :] = jnp.sum(sacc[...].T, axis=0, keepdims=True)
    st_p[plane, 2:3, :] = jnp.sum((pacc[...] * inv[...]).T, axis=0, keepdims=True)
    st_p[plane, 3:4, :] = jnp.zeros((1, NQ), F32)

    def stats_plane(k):
        tx, ty = plane_peer(k)
        pltpu.make_async_remote_copy(
            st_p.at[plane], st_p.at[plane], sp_s, sp_r, device_id={"x": tx, "y": ty}, device_id_type=MESH
        ).start()

    each(1, NPLANE, stats_plane)
    each(EARLY, MIDDLE, gradients)
    wait_all(st_p.at[pl.ds(0, NPLANE - 1)], sp_s, sp_r)
    peak, total, positive = merged(st_p, NPLANE)
    st_z[z, 0:1, :] = peak
    st_z[z, 1:2, :] = total
    st_z[z, 2:3, :] = positive
    st_z[z, 3:4, :] = jnp.zeros((1, NQ), F32)

    def stats_z(k):
        pltpu.make_async_remote_copy(
            st_z.at[z], st_z.at[z], sz_s, sz_r, device_id={"z": z_peer(k)}, device_id_type=MESH
        ).start()

    each(1, NZ, stats_z)
    each(MIDDLE, SLOTS - 1, gradients)
    new = fresh[...].reshape(SLOT_ROWS, D)
    last = dot(coef[SLOTS - 1], new)
    last_count = dot(cnt[SLOTS - 1], new)
    factor = jnp.exp(mx[...] - top_ref[...])
    for c in range(TILES):
        cols = slice(c * LANES, (c + 1) * LANES)
        gu[:, cols] = (gacc[0:NQ, cols] + gacc[NQ : 2 * NQ, cols]) * factor + (last[0:NQ, cols] + last[NQ : 2 * NQ, cols])
        gt[:, cols] = (gacc[2 * NQ : 3 * NQ, cols] + last_count[:, cols]) * inv[...]
    wait_all(st_z.at[pl.ds(0, NZ - 1)], sz_s, sz_r)
    peak, total, positive = merged(st_z, NZ)
    log_total = peak + jnp.log(total)
    ltb[...] = jnp.exp(top_ref[...] - jnp.broadcast_to(log_total, (LANES, NQ)).T)
    for c in range(TILES):
        cols = slice(c * LANES, (c + 1) * LANES)
        gsend[:, :, cols] = (gu[:, cols] * ltb[...] - gt[:, cols]).astype(BF16).reshape(NPLANE, 2 * NZ, LANES)

    def scatter_plane(k):
        tx, ty = plane_peer(k)
        pltpu.make_async_remote_copy(
            gsend.at[tx * NY + ty], grecv.at[plane], gp_s, gp_r, device_id={"x": tx, "y": ty}, device_id_type=MESH
        ).start()

    each(1, NPLANE, scatter_plane)
    grecv[plane] = gsend[plane]
    loss = log_total - positive
    own = (plane * NZ + z) * 2
    query = lax.broadcasted_iota(I32, (1, NQ), 1)
    for i in range(2):
        loss_ref[:, i : i + 1] = jnp.sum(jnp.where(query == own + i, loss, 0.0), axis=1, keepdims=True)
    wait_all(grecv.at[pl.ds(0, NPLANE - 1)], gp_s, gp_r)
    part = grecv[0].astype(F32)
    for i in range(1, NPLANE):
        part = part + grecv[i].astype(F32)
    hsend[...] = part.reshape(NZ, 2, D)

    def scatter_z(k):
        tz = z_peer(k)
        pltpu.make_async_remote_copy(
            hsend.at[tz], hrecv.at[z], gz_s, gz_r, device_id={"z": tz}, device_id_type=MESH
        ).start()

    each(1, NZ, scatter_z)
    hrecv[z] = hsend[z]
    out_copy.wait()
    wait_all(hrecv.at[pl.ds(0, NZ - 1)], gz_s, gz_r)
    whole = hrecv[0]
    for i in range(1, NZ):
        whole = whole + hrecv[i]
    grad_ref[...] = whole.astype(BF16)


def hand_over(loss_in, grad_in, fresh_in, loss_out, grad_out, fresh_out, held, sems):
    parts = 4
    size = ROWS // parts

    def piece(i):
        return pl.ds(i * size, size)

    ins = [pltpu.make_async_copy(fresh_in.at[piece(i)], held.at[piece(i)], sems.at[0, i]) for i in range(parts)]
    outs = [pltpu.make_async_copy(held.at[piece(i)], fresh_out.at[piece(i)], sems.at[1, i]) for i in range(parts)]
    for copy in ins:
        copy.start()
    loss_out[...] = loss_in[...]
    grad_out[...] = grad_in[...]
    for i in range(parts):
        ins[i].wait()
        outs[i].start()
    for copy in outs:
        copy.wait()


def per_device(
    queries,
    positives,
    label_vectors,
    refresh_slot,
    features,
    encoder_weight,
    encoder_gain,
    free_vectors,
    targets,
):
    vmem = pl.BlockSpec(memory_space=pltpu.VMEM)
    hbm = pl.BlockSpec(memory_space=pl.ANY)
    dma = pltpu.SemaphoreType.DMA
    results = (
        jax.ShapeDtypeStruct((1, 2), F32),
        jax.ShapeDtypeStruct((2, D), BF16),
        jax.ShapeDtypeStruct((ROWS, D), BF16),
    )
    made = pl.pallas_call(
        kernel,
        out_shape=results,
        in_specs=[pl.BlockSpec(memory_space=pltpu.SMEM)] + [hbm] * 8,
        out_specs=(vmem, vmem, hbm),
        scratch_shapes=[
            pltpu.VMEM((2, POS, NQ), I32),
            pltpu.VMEM((ROWS, D), BF16),
            pltpu.VMEM((D, D), BF16),
            pltpu.VMEM((TILES, LANES), F32),
            pltpu.VMEM((2 * NCLS * 3, LANES), I32),
            pltpu.VMEM((NPLANE, NZ, 2, D), BF16),
            pltpu.VMEM((NQ, D), BF16),
            pltpu.VMEM((SLOTS, SLOT_ROWS, D), BF16),
            pltpu.VMEM((ROWS, D), BF16),
            pltpu.VMEM((2 * ROWS, HALF), BF16),
            pltpu.VMEM((NCLS, 2, 3 * HALF), BF16),
            pltpu.VMEM((NCLS, 2, 3 * HALF), BF16),
            pltpu.VMEM((2, ROWS, 3 * 2 * NCLS), BF16),
            pltpu.VMEM((2, ROWS, D), BF16),
            pltpu.VMEM((POS, NQ, LANES), I32),
            pltpu.VMEM((NQ, LANES), F32),
            pltpu.VMEM((SLOTS, NQ, SLOT_ROWS), F32),
            pltpu.VMEM((SLOTS, NQ, SLOT_ROWS), BF16),
            pltpu.VMEM((NQ, LANES), F32),
            pltpu.VMEM((NQ, LANES), F32),
            pltpu.VMEM((NQ, LANES), F32),
            pltpu.VMEM((NQ, LANES), F32),
            pltpu.VMEM((NQ, LANES), F32),
            pltpu.VMEM((SLOTS, 2 * NQ, SLOT_ROWS), BF16),
            pltpu.VMEM((3 * NQ, D), F32),
            pltpu.VMEM((NQ, D), F32),
            pltpu.VMEM((NQ, D), F32),
            pltpu.VMEM((NPLANE, 2 * NZ, D), BF16),
            pltpu.VMEM((NPLANE, 2 * NZ, D), BF16),
            pltpu.VMEM((NZ, 2, D), F32),
            pltpu.VMEM((NZ, 2, D), F32),
            pltpu.VMEM((NPLANE, 4, NQ), F32),
            pltpu.VMEM((NZ, 4, NQ), F32),
            pltpu.SemaphoreType.REGULAR,
        ]
        + [dma] * 6
        + [dma((3,))]
        + [dma] * 6
        + [dma((2,))] * 2
        + [dma] * 8,
        compiler_params=pltpu.CompilerParams(
            collective_id=0, has_side_effects=True, vmem_limit_bytes=56 * 2**20
        ),
    )(
        refresh_slot.reshape(1),
        queries.reshape(2, D),
        jnp.swapaxes(positives, 1, 2),
        label_vectors.reshape(SLOTS, SLOT_ROWS, D),
        features,
        encoder_weight,
        encoder_gain.reshape(TILES, LANES),
        free_vectors,
        targets.reshape(-1, LANES),
    )
    loss, grads, refreshed = pl.pallas_call(
        hand_over,
        out_shape=results,
        in_specs=[vmem, vmem, hbm],
        out_specs=(vmem, vmem, hbm),
        scratch_shapes=[pltpu.VMEM((ROWS, D), BF16), dma((2, 4))],
    )(*made)
    return loss, grads.reshape(1, 2, D), refreshed


def solution(mesh):
    torus = Mesh(mesh.devices.reshape(NY, NZ, NX, mesh.shape["rep"]), CLS_REP)
    placed = (
        P("core", CLS, None),
        P(),
        P(CLS, None),
        P(),
        P(CLS_REP, None),
        P(),
        P(),
        P(CLS_REP, None),
        P(),
    )
    return jax.shard_map(
        per_device,
        mesh=torus,
        in_specs=placed,
        out_specs=(P("core", CLS), P("core", CLS, None), P(CLS_REP, None)),
        check_vma=False,
    )
```

```python
import jax
import jax.numpy as jnp
from jax import lax
from jax.experimental import pallas as pl
from jax.experimental.pallas import tpu as pltpu
from jax.sharding import Mesh
from jax.sharding import PartitionSpec as P

F32 = jnp.float32
BF16 = jnp.bfloat16
I32 = jnp.int32
MESH = pl.DeviceIdType.MESH
CLS = ("y", "z", "x")
CLS_REP = ("y", "z", "x", "core")
NY, NZ, NX = 4, 8, 4
NPLANE = NX * NY
NCLS = NPLANE * NZ
D = 768
HALF = D // 2
ROWS = 384
SLOTS = 8
SLOT_ROWS = 768
LABELS_DEV = SLOTS * SLOT_ROWS
NQ = 256
POS = 4
CHUNK = 32
LANES = 128
TILES = SLOT_ROWS // LANES
EARLY = 2
UNDER_SWAP = 3
FIRST = 21
MIDDLE = 5


def dot(a, b):
    return jnp.dot(a, b, preferred_element_type=F32)


def dot_t(a, b):
    return lax.dot_general(a, b, (((1,), (1,)), ((), ())), preferred_element_type=F32)


def each(lo, hi, fn):
    def step(k, carry):
        fn(k)
        return carry

    lax.fori_loop(lo, hi, step, 0)


def three_of(parts, inside):
    low = high = total = None
    for part, mask in zip(parts, inside):
        lo = jnp.min(jnp.where(mask, part, 1e9), axis=1, keepdims=True)
        hi = jnp.max(jnp.where(mask, part, -1.0), axis=1, keepdims=True)
        su = jnp.sum(jnp.where(mask, part, 0.0), axis=1, keepdims=True)
        low = lo if low is None else jnp.minimum(low, lo)
        high = hi if high is None else jnp.maximum(high, hi)
        total = su if total is None else total + su
    return low, total - low - high, high


def merged(stats, count):
    peak = stats[0, 0:1, :]
    for i in range(1, count):
        peak = jnp.maximum(peak, stats[i, 0:1, :])
    total = jnp.zeros_like(peak)
    positive = jnp.zeros_like(peak)
    for i in range(count):
        total = total + stats[i, 1:2, :] * jnp.exp(stats[i, 0:1, :] - peak)
        positive = positive + stats[i, 2:3, :]
    return peak, total, positive


def kernel(
    slot_hbm, q_hbm, pos_hbm, lab_hbm, feat_hbm, w_hbm, gain_hbm, free_hbm, tgt_hbm,
    loss_ref, grad_ref, fresh_hbm,
    slot_ref, pos_ref, feat_ref, w_ref, gain_ref, tgt_ref,
    qg, qm, lab, free, enc2, send, recv, put, fresh, off, inv, lg, cnt, mx, top_ref, sacc, pacc, ltb, coef, gacc, gcnt, gu, gt,
    gsend, grecv, hsend, hrecv, st_p, st_z,
    ready,
    lab_sem, free_sem, q_sem, out_sem, w_sem, feat_sem, small_sem,
    qz_s, qz_r, qp_s, qp_r, d_s, d_r, f_s, f_r, sp_s, sp_r, sz_s, sz_r, gp_s, gp_r, gz_s, gz_r,
):
    y, z, x = lax.axis_index("y"), lax.axis_index("z"), lax.axis_index("x")
    core = lax.axis_index("core")
    me = (y * NZ + z) * NX + x
    plane = x * NY + y

    def z_peer(k):
        return (z + k) % NZ

    def plane_peer(k):
        return (x + k // NY) % NX, (y + k % NY) % NY

    def wait_all(ref, s, r):
        pltpu.make_async_copy(ref, ref, r).wait()
        pltpu.make_async_copy(ref, ref, s).wait()

    barrier = pltpu.get_barrier_semaphore()

    def greet_z(k):
        pl.semaphore_signal(barrier, inc=1, device_id={"z": z_peer(k)}, device_id_type=MESH)

    def greet_plane(k):
        tx, ty = plane_peer(k)
        pl.semaphore_signal(barrier, inc=1, device_id={"x": tx, "y": ty}, device_id_type=MESH)

    each(1, NZ, greet_z)
    each(1, NPLANE, greet_plane)
    pl.semaphore_signal(barrier, inc=1, device_id={"core": 1 - core}, device_id_type=MESH)

    q_copy = pltpu.make_async_copy(q_hbm, qg.at[plane, z], q_sem)
    w_copy = pltpu.make_async_copy(w_hbm, w_ref, w_sem)
    feat_copy = pltpu.make_async_copy(feat_hbm, feat_ref, feat_sem)
    gain_copy = pltpu.make_async_copy(gain_hbm, gain_ref, small_sem.at[0])
    pos_copy = pltpu.make_async_copy(pos_hbm, pos_ref, small_sem.at[1])
    tgt_copy = pltpu.make_async_copy(tgt_hbm, tgt_ref, small_sem.at[2])
    free_copy = pltpu.make_async_copy(free_hbm, free, free_sem)
    lab_copy = pltpu.make_async_copy(lab_hbm, lab, lab_sem)
    slot_copy = pltpu.make_async_copy(slot_hbm, slot_ref, small_sem.at[3])
    for copy in (w_copy, feat_copy, gain_copy, tgt_copy, q_copy, pos_copy, slot_copy, free_copy, lab_copy):
        copy.start()

    w_copy.wait()
    feat_copy.wait()
    gain_copy.wait()
    hidden = dot(feat_ref[...], w_ref[...])
    scale = lax.rsqrt(jnp.mean(hidden * hidden, axis=1, keepdims=True) + 1e-06)
    for c in range(2):
        for j in range(TILES // 2):
            i = c * (TILES // 2) + j
            cols = hidden[:, i * LANES : (i + 1) * LANES] * scale * gain_ref[i : i + 1, :]
            enc2[c * ROWS : (c + 1) * ROWS, j * LANES : (j + 1) * LANES] = cols.astype(BF16)

    tgt_copy.wait()
    block = me * 2 + core
    row = lax.broadcasted_iota(I32, (2 * NCLS, LANES), 0)
    owner_base = (row // 2) * SLOT_ROWS
    parts = []
    inside = []
    for k in range(3):
        part = tgt_ref[pl.ds(3 * block + k, 1), :] - owner_base
        parts.append(part.astype(F32))
        inside.append((part >= 0) & (part < SLOT_ROWS))
    picks = three_of(parts, inside)
    even = row % 2 == 0
    for r in range(3):
        hit = [part == picks[r] for part in parts]
        one = [jnp.where(h & even, 1.0, 0.0).astype(BF16) for h in hit]
        two = [jnp.where(h & ~even, 1.0, 0.0).astype(BF16) for h in hit]
        chosen = dot(jnp.concatenate(one + two, axis=1), enc2[...])
        send[:, :, r * HALF : (r + 1) * HALF] = chosen.astype(BF16).reshape(NCLS, 2, HALF)

    q_copy.wait()
    pl.semaphore_wait(barrier, NZ - 1 + NPLANE - 1 + 1)

    def ready_z(k):
        pl.semaphore_signal(ready, inc=1, device_id={"z": z_peer(k)}, device_id_type=MESH)

    def gather_z(k):
        pltpu.make_async_remote_copy(
            qg.at[plane, z], qg.at[plane, z], qz_s, qz_r, device_id={"z": z_peer(k)}, device_id_type=MESH
        ).start()

    each(1, NZ, ready_z)
    each(1, NZ, gather_z)

    def gather_plane(k):
        tx, ty = plane_peer(k)
        pltpu.make_async_remote_copy(
            qg.at[plane], qg.at[plane], qp_s, qp_r, device_id={"x": tx, "y": ty}, device_id_type=MESH
        ).start()

    def dispatch(dz, j):
        tz = z_peer(dz)
        tx, ty = plane_peer(j)
        dest = (ty * NZ + tz) * NX + tx
        pltpu.make_async_remote_copy(
            send.at[dest], recv.at[me], d_s, d_r, device_id={"y": ty, "z": tz, "x": tx}, device_id_type=MESH
        ).start()

    def dispatch_far(k):
        dispatch(1 + k % (NZ - 1), 1 + k // (NZ - 1))

    each(1, NZ, lambda k: dispatch(k, 0))
    each(1, NPLANE, lambda j: dispatch(0, j))
    pl.semaphore_wait(ready, NZ - 1)
    far = (NZ - 1) * (NPLANE - 1)
    each(0, FIRST, dispatch_far)
    wait_all(qg.at[plane, pl.ds(0, NZ - 1)], qz_s, qz_r)
    each(1, NPLANE, gather_plane)
    each(FIRST, far, dispatch_far)
    recv[me] = send[me]

    parts = []
    inside = []
    for k in range(3):
        first = tgt_ref[pl.ds(k, NCLS, stride=6), :]
        second = tgt_ref[pl.ds(3 + k, NCLS, stride=6), :]
        part = jnp.where(core == 0, first, second) - (me * SLOT_ROWS + core * ROWS)
        parts.append(part.astype(F32))
        inside.append((part >= 0) & (part < ROWS))
    picks = three_of(parts, inside)
    lane = lax.broadcasted_iota(I32, (NCLS, ROWS), 1).astype(F32)
    spread_row = lax.broadcasted_iota(I32, (NCLS, 2 * NCLS), 0) * 2
    spread_col = lax.broadcasted_iota(I32, (NCLS, 2 * NCLS), 1)
    for r in range(3):
        to_row = jnp.where(lane == picks[r], 1.0, 0.0).T.astype(BF16)
        for c in range(2):
            spread = jnp.where(spread_col == spread_row + c, 1.0, 0.0).astype(BF16)
            put[c, :, r * 2 * NCLS : (r + 1) * 2 * NCLS] = dot(to_row, spread).astype(BF16)

    pos_copy.wait()
    slot_copy.wait()
    slot = slot_ref[0]
    q_row = lax.broadcasted_iota(I32, (NQ, NQ), 0)
    q_col = lax.broadcasted_iota(I32, (NQ, NQ), 1)
    natural = ((((q_row // 16) % NY) * NZ + (q_row // 2) % NZ) * NX + q_row // 64) * 2 + q_row % 2
    order = jnp.where(q_col == natural, 1.0, 0.0).astype(BF16)
    ids = pos_ref[core] + 1
    ids = sum(
        dot_t(order, ((ids >> (8 * i)) & 255).astype(F32).astype(BF16)) * float(256**i) for i in range(3)
    )
    valid = ids >= 1.0
    count = jnp.sum(jnp.where(valid, 1.0, 0.0), axis=1, keepdims=True)
    inv[...] = jnp.broadcast_to(1.0 / count, (NQ, LANES))
    local = jnp.where(valid, ids.astype(I32) - (1 + me * LABELS_DEV), -LABELS_DEV)
    for j in range(POS):
        off[j] = jnp.broadcast_to(local[:, j : j + 1], (NQ, LANES))

    def slot_of(k):
        return lax.rem(slot + 1 + k, SLOTS)

    nblocks = NQ // CHUNK

    def counts(k):
        base = slot_of(k) * SLOT_ROWS

        def rows(b):
            at = pl.ds(b * CHUNK, CHUNK)
            lane_id = lax.broadcasted_iota(I32, (CHUNK, LANES), 1) + base
            offs = [off[j, at, :] - lane_id for j in range(POS)]
            for c in range(TILES):
                acc = jnp.zeros((CHUNK, LANES), F32)
                for j in range(POS):
                    acc = acc + jnp.where(offs[j] == c * LANES, 1.0, 0.0)
                cnt[k, at, c * LANES : (c + 1) * LANES] = acc.astype(BF16)

        each(0, nblocks, rows)

    each(0, SLOTS, counts)

    lab_copy.wait()
    gcnt[...] = dot(cnt[0], lab[slot_of(0)])

    def count_rows(k):
        gcnt[...] += dot(cnt[k], lab[slot_of(k)])

    each(1, SLOTS - 1, count_rows)
    wait_all(qg.at[pl.ds(0, NPLANE - 1)], qp_s, qp_r)
    qm[...] = qg[...].reshape(NQ, D)

    def highest(values):
        top = values[:, 0:LANES]
        for c in range(1, values.shape[1] // LANES):
            top = jnp.maximum(top, values[:, c * LANES : (c + 1) * LANES])
        return top

    def logits_of(k, peak):
        values = dot_t(qm[...], lab[slot_of(k)])
        lg[k] = values
        return jnp.maximum(peak, highest(values))

    peak = lax.fori_loop(0, SLOTS - 1, logits_of, jnp.full((NQ, LANES), -jnp.inf, F32))
    mx[...] = jnp.broadcast_to(jnp.max(peak, axis=1, keepdims=True), (NQ, LANES))
    sacc[...] = jnp.zeros((NQ, LANES), F32)
    positive = jnp.zeros((NQ, LANES), F32)
    for c in range(TILES):
        cols = slice(c * LANES, (c + 1) * LANES)
        positive = positive + qm[:, cols].astype(F32) * gcnt[:, cols]
    pacc[...] = positive

    def weights(k, level_ref):
        def rows(b):
            at = pl.ds(b * CHUNK, CHUNK)
            low_at = pl.ds(NQ + b * CHUNK, CHUNK)
            level = level_ref[at, :]
            s = sacc[at, :]
            for c in range(TILES):
                cols = slice(c * LANES, (c + 1) * LANES)
                e = jnp.exp(lg[k, at, cols] - level)
                s = s + e
                high = e.astype(BF16)
                coef[k, at, cols] = high
                coef[k, low_at, cols] = (e - high.astype(F32)).astype(BF16)
            sacc[at, :] = s

        each(0, nblocks, rows)

    each(0, SLOTS - 1, lambda k: weights(k, mx))
    gacc[...] = dot(coef[0], lab[slot_of(0)])

    def gradients(k):
        gacc[...] += dot(coef[k], lab[slot_of(k)])

    each(1, EARLY, gradients)

    free_copy.wait()
    wait_all(recv.at[pl.ds(0, NCLS - 1)], d_s, d_r)
    arrived = recv[...].reshape(2 * NCLS, 3 * HALF)
    stacked = jnp.concatenate([arrived[:, r * HALF : (r + 1) * HALF] for r in range(3)], axis=0)
    swaps = []
    for h in range(2):
        at = slice(h * (ROWS // 2), (h + 1) * (ROWS // 2))
        for c in range(2):
            cols = slice(c * HALF, (c + 1) * HALF)
            fresh[core, at, cols] = (free[at, cols].astype(F32) + dot(put[c, at, :], stacked)).astype(BF16)
        swap = pltpu.make_async_remote_copy(
            fresh.at[core, at], fresh.at[core, at], f_s.at[h], f_r.at[h],
            device_id={"core": 1 - core}, device_id_type=MESH,
        )
        swap.start()
        swaps.append(swap)
    out_copy = pltpu.make_async_copy(fresh.at[core], fresh_hbm, out_sem)
    out_copy.start()
    own_logits = dot_t(qm[...], fresh[core])
    each(EARLY, UNDER_SWAP, gradients)
    for swap in swaps:
        swap.wait()
    other_logits = dot_t(qm[...], fresh[1 - core])
    peak = jnp.maximum(highest(own_logits), highest(other_logits))
    lg[SLOTS - 1, :, 0:ROWS] = jnp.where(core == 0, own_logits, other_logits)
    lg[SLOTS - 1, :, ROWS : 2 * ROWS] = jnp.where(core == 0, other_logits, own_logits)
    old = mx[...]
    top = jnp.maximum(old, jnp.broadcast_to(jnp.max(peak, axis=1, keepdims=True), (NQ, LANES)))
    sacc[...] = sacc[...] * jnp.exp(old - top)
    top_ref[...] = top
    weights(SLOTS - 1, top_ref)
    positive = pacc[...]
    for c in range(TILES):
        cols = slice(c * LANES, (c + 1) * LANES)
        positive = positive + cnt[SLOTS - 1, :, cols].astype(F32) * lg[SLOTS - 1, :, cols]
    pacc[...] = positive

    st_p[plane, 0:1, :] = top_ref[...].T[0:1, :]
    st_p[plane, 1:2, :] = jnp.sum(sacc[...].T, axis=0, keepdims=True)
    st_p[plane, 2:3, :] = jnp.sum((pacc[...] * inv[...]).T, axis=0, keepdims=True)
    st_p[plane, 3:4, :] = jnp.zeros((1, NQ), F32)

    def stats_plane(k):
        tx, ty = plane_peer(k)
        pltpu.make_async_remote_copy(
            st_p.at[plane], st_p.at[plane], sp_s, sp_r, device_id={"x": tx, "y": ty}, device_id_type=MESH
        ).start()

    each(1, NPLANE, stats_plane)
    each(UNDER_SWAP, MIDDLE, gradients)
    wait_all(st_p.at[pl.ds(0, NPLANE - 1)], sp_s, sp_r)
    peak, total, positive = merged(st_p, NPLANE)
    st_z[z, 0:1, :] = peak
    st_z[z, 1:2, :] = total
    st_z[z, 2:3, :] = positive
    st_z[z, 3:4, :] = jnp.zeros((1, NQ), F32)

    def stats_z(k):
        pltpu.make_async_remote_copy(
            st_z.at[z], st_z.at[z], sz_s, sz_r, device_id={"z": z_peer(k)}, device_id_type=MESH
        ).start()

    each(1, NZ, stats_z)
    each(MIDDLE, SLOTS - 1, gradients)
    new = fresh[...].reshape(SLOT_ROWS, D)
    last = dot(coef[SLOTS - 1], new)
    last_count = dot(cnt[SLOTS - 1], new)
    factor = jnp.exp(mx[...] - top_ref[...])
    for c in range(TILES):
        cols = slice(c * LANES, (c + 1) * LANES)
        gu[:, cols] = (gacc[0:NQ, cols] + gacc[NQ : 2 * NQ, cols]) * factor + (last[0:NQ, cols] + last[NQ : 2 * NQ, cols])
        gt[:, cols] = (gcnt[:, cols] + last_count[:, cols]) * inv[...]
    wait_all(st_z.at[pl.ds(0, NZ - 1)], sz_s, sz_r)
    peak, total, positive = merged(st_z, NZ)
    log_total = peak + jnp.log(total)
    ltb[...] = jnp.exp(top_ref[...] - jnp.broadcast_to(log_total, (LANES, NQ)).T)
    for c in range(TILES):
        cols = slice(c * LANES, (c + 1) * LANES)
        gsend[:, :, cols] = (gu[:, cols] * ltb[...] - gt[:, cols]).astype(BF16).reshape(NPLANE, 2 * NZ, LANES)

    def scatter_plane(k):
        tx, ty = plane_peer(k)
        pltpu.make_async_remote_copy(
            gsend.at[tx * NY + ty], grecv.at[plane], gp_s, gp_r, device_id={"x": tx, "y": ty}, device_id_type=MESH
        ).start()

    each(1, NPLANE, scatter_plane)
    grecv[plane] = gsend[plane]
    loss = log_total - positive
    own = (plane * NZ + z) * 2
    query = lax.broadcasted_iota(I32, (1, NQ), 1)
    for i in range(2):
        loss_ref[:, i : i + 1] = jnp.sum(jnp.where(query == own + i, loss, 0.0), axis=1, keepdims=True)
    wait_all(grecv.at[pl.ds(0, NPLANE - 1)], gp_s, gp_r)
    part = grecv[0].astype(F32)
    for i in range(1, NPLANE):
        part = part + grecv[i].astype(F32)
    hsend[...] = part.reshape(NZ, 2, D)

    def scatter_z(k):
        tz = z_peer(k)
        pltpu.make_async_remote_copy(
            hsend.at[tz], hrecv.at[z], gz_s, gz_r, device_id={"z": tz}, device_id_type=MESH
        ).start()

    each(1, NZ, scatter_z)
    hrecv[z] = hsend[z]
    out_copy.wait()
    wait_all(hrecv.at[pl.ds(0, NZ - 1)], gz_s, gz_r)
    whole = hrecv[0]
    for i in range(1, NZ):
        whole = whole + hrecv[i]
    grad_ref[...] = whole.astype(BF16)


def hand_over(loss_in, grad_in, fresh_in, loss_out, grad_out, fresh_out, loss, grad, fresh, sems):
    parts = 2
    size = ROWS // parts
    moves = [(loss_in, loss, loss_out), (grad_in, grad, grad_out)]
    for i in range(parts):
        at = pl.ds(i * size, size)
        moves.append((fresh_in.at[at], fresh.at[at], fresh_out.at[at]))
    ins = [pltpu.make_async_copy(a, b, sems.at[0, i]) for i, (a, b, _) in enumerate(moves)]
    outs = [pltpu.make_async_copy(b, c, sems.at[1, i]) for i, (_, b, c) in enumerate(moves)]
    for copy in ins:
        copy.start()
    for i in range(len(moves)):
        ins[i].wait()
        outs[i].start()
    for copy in outs:
        copy.wait()


def per_device(
    queries,
    positives,
    label_vectors,
    refresh_slot,
    features,
    encoder_weight,
    encoder_gain,
    free_vectors,
    targets,
):
    vmem = pl.BlockSpec(memory_space=pltpu.VMEM)
    hbm = pl.BlockSpec(memory_space=pl.ANY)
    dma = pltpu.SemaphoreType.DMA
    results = (
        jax.ShapeDtypeStruct((1, 2), F32),
        jax.ShapeDtypeStruct((2, D), BF16),
        jax.ShapeDtypeStruct((ROWS, D), BF16),
    )
    made = pl.pallas_call(
        kernel,
        out_shape=results,
        in_specs=[hbm] * 9,
        out_specs=(vmem, vmem, hbm),
        scratch_shapes=[
            pltpu.SMEM((1,), I32),
            pltpu.VMEM((2, POS, NQ), I32),
            pltpu.VMEM((ROWS, D), BF16),
            pltpu.VMEM((D, D), BF16),
            pltpu.VMEM((TILES, LANES), F32),
            pltpu.VMEM((2 * NCLS * 3, LANES), I32),
            pltpu.VMEM((NPLANE, NZ, 2, D), BF16),
            pltpu.VMEM((NQ, D), BF16),
            pltpu.VMEM((SLOTS, SLOT_ROWS, D), BF16),
            pltpu.VMEM((ROWS, D), BF16),
            pltpu.VMEM((2 * ROWS, HALF), BF16),
            pltpu.VMEM((NCLS, 2, 3 * HALF), BF16),
            pltpu.VMEM((NCLS, 2, 3 * HALF), BF16),
            pltpu.VMEM((2, ROWS, 3 * 2 * NCLS), BF16),
            pltpu.VMEM((2, ROWS, D), BF16),
            pltpu.VMEM((POS, NQ, LANES), I32),
            pltpu.VMEM((NQ, LANES), F32),
            pltpu.VMEM((SLOTS, NQ, SLOT_ROWS), F32),
            pltpu.VMEM((SLOTS, NQ, SLOT_ROWS), BF16),
            pltpu.VMEM((NQ, LANES), F32),
            pltpu.VMEM((NQ, LANES), F32),
            pltpu.VMEM((NQ, LANES), F32),
            pltpu.VMEM((NQ, LANES), F32),
            pltpu.VMEM((NQ, LANES), F32),
            pltpu.VMEM((SLOTS, 2 * NQ, SLOT_ROWS), BF16),
            pltpu.VMEM((2 * NQ, D), F32),
            pltpu.VMEM((NQ, D), F32),
            pltpu.VMEM((NQ, D), F32),
            pltpu.VMEM((NQ, D), F32),
            pltpu.VMEM((NPLANE, 2 * NZ, D), BF16),
            pltpu.VMEM((NPLANE, 2 * NZ, D), BF16),
            pltpu.VMEM((NZ, 2, D), F32),
            pltpu.VMEM((NZ, 2, D), F32),
            pltpu.VMEM((NPLANE, 4, NQ), F32),
            pltpu.VMEM((NZ, 4, NQ), F32),
            pltpu.SemaphoreType.REGULAR,
        ]
        + [dma] * 6
        + [dma((4,))]
        + [dma] * 6
        + [dma((2,))] * 2
        + [dma] * 8,
        compiler_params=pltpu.CompilerParams(
            collective_id=0, has_side_effects=True, vmem_limit_bytes=56 * 2**20
        ),
    )(
        refresh_slot.reshape(1),
        queries.reshape(2, D),
        jnp.swapaxes(positives, 1, 2),
        label_vectors.reshape(SLOTS, SLOT_ROWS, D),
        features,
        encoder_weight,
        encoder_gain.reshape(TILES, LANES),
        free_vectors,
        targets.reshape(-1, LANES),
    )
    loss, grads, refreshed = pl.pallas_call(
        hand_over,
        out_shape=results,
        in_specs=[hbm] * 3,
        out_specs=(hbm,) * 3,
        scratch_shapes=[
            pltpu.VMEM((1, 2), F32),
            pltpu.VMEM((2, D), BF16),
            pltpu.VMEM((ROWS, D), BF16),
            dma((2, 4)),
        ],
    )(*made)
    return loss, grads.reshape(1, 2, D), refreshed


def solution(mesh):
    torus = Mesh(mesh.devices.reshape(NY, NZ, NX, mesh.shape["rep"]), CLS_REP)
    placed = (
        P("core", CLS, None),
        P(),
        P(CLS, None),
        P(),
        P(CLS_REP, None),
        P(),
        P(),
        P(CLS_REP, None),
        P(),
    )
    return jax.shard_map(
        per_device,
        mesh=torus,
        in_specs=placed,
        out_specs=(P("core", CLS), P("core", CLS, None), P(CLS_REP, None)),
        check_vma=False,
    )
```

```python
import jax
import jax.numpy as jnp
from jax import lax
from jax.experimental import pallas as pl
from jax.experimental.pallas import tpu as pltpu
from jax.sharding import Mesh
from jax.sharding import PartitionSpec as P

F32 = jnp.float32
BF16 = jnp.bfloat16
I32 = jnp.int32
MESH = pl.DeviceIdType.MESH
CLS = ("y", "z", "x")
CLS_REP = ("y", "z", "x", "core")
NY, NZ, NX = 4, 8, 4
NPLANE = NX * NY
NCLS = NPLANE * NZ
D = 768
HALF = D // 2
ROWS = 384
SLOTS = 8
SLOT_ROWS = 768
LABELS_DEV = SLOTS * SLOT_ROWS
NQ = 256
POS = 4
CHUNK = 32
LANES = 128
TILES = SLOT_ROWS // LANES
EARLY = 2
UNDER_SWAP = 3
FIRST = 4
MIDDLE = 5


def dot(a, b):
    return jnp.dot(a, b, preferred_element_type=F32)


def dot_t(a, b):
    return lax.dot_general(a, b, (((1,), (1,)), ((), ())), preferred_element_type=F32)


def each(lo, hi, fn):
    def step(k, carry):
        fn(k)
        return carry

    lax.fori_loop(lo, hi, step, 0)


def three_of(parts, inside):
    low = high = total = None
    for part, mask in zip(parts, inside):
        lo = jnp.min(jnp.where(mask, part, 1e9), axis=1, keepdims=True)
        hi = jnp.max(jnp.where(mask, part, -1.0), axis=1, keepdims=True)
        su = jnp.sum(jnp.where(mask, part, 0.0), axis=1, keepdims=True)
        low = lo if low is None else jnp.minimum(low, lo)
        high = hi if high is None else jnp.maximum(high, hi)
        total = su if total is None else total + su
    return low, total - low - high, high


def merged(stats, count):
    peak = stats[0, 0:1, :]
    for i in range(1, count):
        peak = jnp.maximum(peak, stats[i, 0:1, :])
    total = jnp.zeros_like(peak)
    positive = jnp.zeros_like(peak)
    for i in range(count):
        total = total + stats[i, 1:2, :] * jnp.exp(stats[i, 0:1, :] - peak)
        positive = positive + stats[i, 2:3, :]
    return peak, total, positive


def kernel(
    slot_hbm, q_hbm, pos_hbm, lab_hbm, feat_hbm, w_hbm, gain_hbm, free_hbm, tgt_hbm,
    loss_ref, grad_ref, fresh_hbm,
    slot_ref, pos_ref, feat_ref, w_ref, gain_ref, tgt_ref,
    qg, qm, lab, free, enc2, send, recv, put, fresh, off, inv, lg, cnt, mx, top_ref, sacc, pacc, ltb, coef, gacc, gcnt, gu, gt,
    gsend, grecv, hsend, hrecv, st_p, st_z,
    ready,
    lab_sem, free_sem, q_sem, out_sem, w_sem, feat_sem, small_sem,
    qz_s, qz_r, qp_s, qp_r, d_s, d_r, f_s, f_r, sp_s, sp_r, sz_s, sz_r, gp_s, gp_r, gz_s, gz_r,
):
    y, z, x = lax.axis_index("y"), lax.axis_index("z"), lax.axis_index("x")
    core = lax.axis_index("core")
    me = (y * NZ + z) * NX + x
    plane = x * NY + y

    def z_peer(k):
        return lax.rem(z + k, NZ)

    def plane_peer(k):
        return lax.rem(x + lax.div(k, NY), NX), lax.rem(y + lax.rem(k, NY), NY)

    def wait_all(ref, s, r):
        pltpu.make_async_copy(ref, ref, r).wait()
        pltpu.make_async_copy(ref, ref, s).wait()

    barrier = pltpu.get_barrier_semaphore()

    def greet_z(k):
        pl.semaphore_signal(barrier, inc=1, device_id={"z": z_peer(k)}, device_id_type=MESH)

    def greet_plane(k):
        tx, ty = plane_peer(k)
        pl.semaphore_signal(barrier, inc=1, device_id={"x": tx, "y": ty}, device_id_type=MESH)

    each(1, NZ, greet_z)
    each(1, NPLANE, greet_plane)
    pl.semaphore_signal(barrier, inc=1, device_id={"core": 1 - core}, device_id_type=MESH)

    q_copy = pltpu.make_async_copy(q_hbm, qg.at[plane, z], q_sem)
    w_copy = pltpu.make_async_copy(w_hbm, w_ref, w_sem)
    feat_copy = pltpu.make_async_copy(feat_hbm, feat_ref, feat_sem)
    gain_copy = pltpu.make_async_copy(gain_hbm, gain_ref, small_sem.at[0])
    pos_copy = pltpu.make_async_copy(pos_hbm, pos_ref, small_sem.at[1])
    tgt_copy = pltpu.make_async_copy(tgt_hbm, tgt_ref, small_sem.at[2])
    free_copy = pltpu.make_async_copy(free_hbm, free, free_sem)
    lab_copy = pltpu.make_async_copy(lab_hbm, lab, lab_sem)
    slot_copy = pltpu.make_async_copy(slot_hbm, slot_ref, small_sem.at[3])
    for copy in (w_copy, feat_copy, gain_copy, tgt_copy, q_copy, pos_copy, slot_copy, free_copy, lab_copy):
        copy.start()

    w_copy.wait()
    feat_copy.wait()
    gain_copy.wait()
    hidden = dot(feat_ref[...], w_ref[...])
    scale = lax.rsqrt(jnp.mean(hidden * hidden, axis=1, keepdims=True) + 1e-06)
    for c in range(2):
        for j in range(TILES // 2):
            i = c * (TILES // 2) + j
            cols = hidden[:, i * LANES : (i + 1) * LANES] * scale * gain_ref[i : i + 1, :]
            enc2[c * ROWS : (c + 1) * ROWS, j * LANES : (j + 1) * LANES] = cols.astype(BF16)

    tgt_copy.wait()
    block = me * 2 + core
    row = lax.broadcasted_iota(I32, (2 * NCLS, LANES), 0)
    owner_base = (row // 2) * SLOT_ROWS
    parts = []
    inside = []
    for k in range(3):
        part = tgt_ref[pl.ds(3 * block + k, 1), :] - owner_base
        parts.append(part.astype(F32))
        inside.append((part >= 0) & (part < SLOT_ROWS))
    picks = three_of(parts, inside)
    even = row % 2 == 0
    for r in range(3):
        hit = [part == picks[r] for part in parts]
        one = [jnp.where(h & even, 1.0, 0.0).astype(BF16) for h in hit]
        two = [jnp.where(h & ~even, 1.0, 0.0).astype(BF16) for h in hit]
        chosen = dot(jnp.concatenate(one + two, axis=1), enc2[...])
        send[:, :, r * HALF : (r + 1) * HALF] = chosen.astype(BF16).reshape(NCLS, 2, HALF)

    q_copy.wait()
    pl.semaphore_wait(barrier, NZ - 1 + NPLANE - 1 + 1)

    def ready_z(k):
        pl.semaphore_signal(ready, inc=1, device_id={"z": z_peer(k)}, device_id_type=MESH)

    def gather_z(k):
        pltpu.make_async_remote_copy(
            qg.at[plane, z], qg.at[plane, z], qz_s, qz_r, device_id={"z": z_peer(k)}, device_id_type=MESH
        ).start()

    each(1, NZ, ready_z)
    each(1, NZ, gather_z)

    def gather_plane(k):
        tx, ty = plane_peer(k)
        pltpu.make_async_remote_copy(
            qg.at[plane], qg.at[plane], qp_s, qp_r, device_id={"x": tx, "y": ty}, device_id_type=MESH
        ).start()

    def dispatch(dz, j):
        tz = z_peer(dz)
        tx, ty = plane_peer(j)
        dest = (ty * NZ + tz) * NX + tx
        pltpu.make_async_remote_copy(
            send.at[dest], recv.at[me], d_s, d_r, device_id={"y": ty, "z": tz, "x": tx}, device_id_type=MESH
        ).start()

    def dispatch_far(j):
        tx, ty = plane_peer(j)
        for dz in range(1, NZ):
            tz = z_peer(dz)
            dest = (ty * NZ + tz) * NX + tx
            pltpu.make_async_remote_copy(
                send.at[dest], recv.at[me], d_s, d_r, device_id={"y": ty, "z": tz, "x": tx}, device_id_type=MESH
            ).start()

    each(1, NZ, lambda k: dispatch(k, 0))
    each(1, NPLANE, lambda j: dispatch(0, j))

    parts = []
    inside = []
    for k in range(3):
        first = tgt_ref[pl.ds(k, NCLS, stride=6), :]
        second = tgt_ref[pl.ds(3 + k, NCLS, stride=6), :]
        part = jnp.where(core == 0, first, second) - (me * SLOT_ROWS + core * ROWS)
        parts.append(part.astype(F32))
        inside.append((part >= 0) & (part < ROWS))
    picks = three_of(parts, inside)
    lane = lax.broadcasted_iota(I32, (NCLS, ROWS), 1).astype(F32)
    spread_row = lax.broadcasted_iota(I32, (NCLS, 2 * NCLS), 0) * 2
    spread_col = lax.broadcasted_iota(I32, (NCLS, 2 * NCLS), 1)
    for r in range(3):
        to_row = jnp.where(lane == picks[r], 1.0, 0.0).T.astype(BF16)
        for c in range(2):
            spread = jnp.where(spread_col == spread_row + c, 1.0, 0.0).astype(BF16)
            put[c, :, r * 2 * NCLS : (r + 1) * 2 * NCLS] = dot(to_row, spread).astype(BF16)

    pos_copy.wait()
    slot_copy.wait()
    slot = slot_ref[0]
    q_row = lax.broadcasted_iota(I32, (NQ, NQ), 0)
    q_col = lax.broadcasted_iota(I32, (NQ, NQ), 1)
    natural = ((((q_row // 16) % NY) * NZ + (q_row // 2) % NZ) * NX + q_row // 64) * 2 + q_row % 2
    order = jnp.where(q_col == natural, 1.0, 0.0).astype(BF16)
    ids = pos_ref[core] + 1
    ids = sum(
        dot_t(order, ((ids >> (8 * i)) & 255).astype(F32).astype(BF16)) * float(256**i) for i in range(3)
    )
    valid = ids >= 1.0
    count = jnp.sum(jnp.where(valid, 1.0, 0.0), axis=1, keepdims=True)
    inv[...] = jnp.broadcast_to(1.0 / count, (NQ, LANES))
    local = jnp.where(valid, ids.astype(I32) - (1 + me * LABELS_DEV), -LABELS_DEV)
    for j in range(POS):
        off[j] = jnp.broadcast_to(local[:, j : j + 1], (NQ, LANES))

    def slot_of(k):
        return lax.rem(slot + 1 + k, SLOTS)

    nblocks = NQ // CHUNK

    def counts(k):
        base = slot_of(k) * SLOT_ROWS

        def rows(b):
            at = pl.ds(b * CHUNK, CHUNK)
            lane_id = lax.broadcasted_iota(I32, (CHUNK, LANES), 1) + base
            offs = [off[j, at, :] - lane_id for j in range(POS)]
            for c in range(TILES):
                acc = jnp.zeros((CHUNK, LANES), F32)
                for j in range(POS):
                    acc = acc + jnp.where(offs[j] == c * LANES, 1.0, 0.0)
                cnt[k, at, c * LANES : (c + 1) * LANES] = acc.astype(BF16)

        each(0, nblocks, rows)

    each(0, SLOTS, counts)

    pl.semaphore_wait(ready, NZ - 1)
    each(1, FIRST, dispatch_far)
    wait_all(qg.at[plane, pl.ds(0, NZ - 1)], qz_s, qz_r)
    each(1, NPLANE, gather_plane)
    each(FIRST, NPLANE, dispatch_far)
    recv[me] = send[me]

    lab_copy.wait()
    gcnt[...] = dot(cnt[0], lab[slot_of(0)])

    def count_rows(k):
        gcnt[...] += dot(cnt[k], lab[slot_of(k)])

    each(1, SLOTS - 1, count_rows)
    wait_all(qg.at[pl.ds(0, NPLANE - 1)], qp_s, qp_r)
    qm[...] = qg[...].reshape(NQ, D)

    def highest(values):
        top = values[:, 0:LANES]
        for c in range(1, values.shape[1] // LANES):
            top = jnp.maximum(top, values[:, c * LANES : (c + 1) * LANES])
        return top

    def logits_of(k, peak):
        values = dot_t(qm[...], lab[slot_of(k)])
        lg[k] = values
        return jnp.maximum(peak, highest(values))

    peak = lax.fori_loop(0, SLOTS - 1, logits_of, jnp.full((NQ, LANES), -jnp.inf, F32))
    mx[...] = jnp.broadcast_to(jnp.max(peak, axis=1, keepdims=True), (NQ, LANES))
    sacc[...] = jnp.zeros((NQ, LANES), F32)
    positive = jnp.zeros((NQ, LANES), F32)
    for c in range(TILES):
        cols = slice(c * LANES, (c + 1) * LANES)
        positive = positive + qm[:, cols].astype(F32) * gcnt[:, cols]
    pacc[...] = positive

    def weights(k, level_ref):
        def rows(b):
            at = pl.ds(b * CHUNK, CHUNK)
            low_at = pl.ds(NQ + b * CHUNK, CHUNK)
            level = level_ref[at, :]
            s = sacc[at, :]
            for c in range(TILES):
                cols = slice(c * LANES, (c + 1) * LANES)
                e = jnp.exp(lg[k, at, cols] - level)
                s = s + e
                high = e.astype(BF16)
                coef[k, at, cols] = high
                coef[k, low_at, cols] = (e - high.astype(F32)).astype(BF16)
            sacc[at, :] = s

        each(0, nblocks, rows)

    each(0, SLOTS - 1, lambda k: weights(k, mx))
    gacc[...] = dot(coef[0], lab[slot_of(0)])

    def gradients(k):
        gacc[...] += dot(coef[k], lab[slot_of(k)])

    each(1, EARLY, gradients)

    free_copy.wait()
    wait_all(recv.at[pl.ds(0, NCLS - 1)], d_s, d_r)
    arrived = recv[...].reshape(2 * NCLS, 3 * HALF)
    stacked = jnp.concatenate([arrived[:, r * HALF : (r + 1) * HALF] for r in range(3)], axis=0)
    swaps = []
    for h in range(2):
        at = slice(h * (ROWS // 2), (h + 1) * (ROWS // 2))
        for c in range(2):
            cols = slice(c * HALF, (c + 1) * HALF)
            fresh[core, at, cols] = (free[at, cols].astype(F32) + dot(put[c, at, :], stacked)).astype(BF16)
        swap = pltpu.make_async_remote_copy(
            fresh.at[core, at], fresh.at[core, at], f_s.at[h], f_r.at[h],
            device_id={"core": 1 - core}, device_id_type=MESH,
        )
        swap.start()
        swaps.append(swap)
    out_copy = pltpu.make_async_copy(fresh.at[core], fresh_hbm, out_sem)
    out_copy.start()
    own_logits = dot_t(qm[...], fresh[core])
    each(EARLY, UNDER_SWAP, gradients)
    for swap in swaps:
        swap.wait()
    other_logits = dot_t(qm[...], fresh[1 - core])
    peak = jnp.maximum(highest(own_logits), highest(other_logits))
    lg[SLOTS - 1, :, 0:ROWS] = jnp.where(core == 0, own_logits, other_logits)
    lg[SLOTS - 1, :, ROWS : 2 * ROWS] = jnp.where(core == 0, other_logits, own_logits)
    old = mx[...]
    top = jnp.maximum(old, jnp.broadcast_to(jnp.max(peak, axis=1, keepdims=True), (NQ, LANES)))
    sacc[...] = sacc[...] * jnp.exp(old - top)
    top_ref[...] = top
    weights(SLOTS - 1, top_ref)
    positive = pacc[...]
    for c in range(TILES):
        cols = slice(c * LANES, (c + 1) * LANES)
        positive = positive + cnt[SLOTS - 1, :, cols].astype(F32) * lg[SLOTS - 1, :, cols]
    pacc[...] = positive

    st_p[plane, 0:1, :] = top_ref[...].T[0:1, :]
    st_p[plane, 1:2, :] = jnp.sum(sacc[...].T, axis=0, keepdims=True)
    st_p[plane, 2:3, :] = jnp.sum((pacc[...] * inv[...]).T, axis=0, keepdims=True)
    st_p[plane, 3:4, :] = jnp.zeros((1, NQ), F32)

    def stats_plane(k):
        tx, ty = plane_peer(k)
        pltpu.make_async_remote_copy(
            st_p.at[plane], st_p.at[plane], sp_s, sp_r, device_id={"x": tx, "y": ty}, device_id_type=MESH
        ).start()

    each(1, NPLANE, stats_plane)
    each(UNDER_SWAP, MIDDLE, gradients)
    wait_all(st_p.at[pl.ds(0, NPLANE - 1)], sp_s, sp_r)
    peak, total, positive = merged(st_p, NPLANE)
    st_z[z, 0:1, :] = peak
    st_z[z, 1:2, :] = total
    st_z[z, 2:3, :] = positive
    st_z[z, 3:4, :] = jnp.zeros((1, NQ), F32)

    def stats_z(k):
        pltpu.make_async_remote_copy(
            st_z.at[z], st_z.at[z], sz_s, sz_r, device_id={"z": z_peer(k)}, device_id_type=MESH
        ).start()

    each(1, NZ, stats_z)
    each(MIDDLE, SLOTS - 1, gradients)
    new = fresh[...].reshape(SLOT_ROWS, D)
    last = dot(coef[SLOTS - 1], new)
    last_count = dot(cnt[SLOTS - 1], new)
    factor = jnp.exp(mx[...] - top_ref[...])
    for c in range(TILES):
        cols = slice(c * LANES, (c + 1) * LANES)
        gu[:, cols] = (gacc[0:NQ, cols] + gacc[NQ : 2 * NQ, cols]) * factor + (last[0:NQ, cols] + last[NQ : 2 * NQ, cols])
        gt[:, cols] = (gcnt[:, cols] + last_count[:, cols]) * inv[...]
    wait_all(st_z.at[pl.ds(0, NZ - 1)], sz_s, sz_r)
    peak, total, positive = merged(st_z, NZ)
    log_total = peak + jnp.log(total)
    ltb[...] = jnp.exp(top_ref[...] - jnp.broadcast_to(log_total, (LANES, NQ)).T)
    for c in range(TILES):
        cols = slice(c * LANES, (c + 1) * LANES)
        gsend[:, :, cols] = (gu[:, cols] * ltb[...] - gt[:, cols]).astype(BF16).reshape(NPLANE, 2 * NZ, LANES)

    def scatter_plane(k):
        tx, ty = plane_peer(k)
        pltpu.make_async_remote_copy(
            gsend.at[tx * NY + ty], grecv.at[plane], gp_s, gp_r, device_id={"x": tx, "y": ty}, device_id_type=MESH
        ).start()

    each(1, NPLANE, scatter_plane)
    grecv[plane] = gsend[plane]
    loss = log_total - positive
    own = (plane * NZ + z) * 2
    query = lax.broadcasted_iota(I32, (1, NQ), 1)
    for i in range(2):
        loss_ref[:, i : i + 1] = jnp.sum(jnp.where(query == own + i, loss, 0.0), axis=1, keepdims=True)
    wait_all(grecv.at[pl.ds(0, NPLANE - 1)], gp_s, gp_r)
    part = grecv[0].astype(F32)
    for i in range(1, NPLANE):
        part = part + grecv[i].astype(F32)
    hsend[...] = part.reshape(NZ, 2, D)

    def scatter_z(k):
        tz = z_peer(k)
        pltpu.make_async_remote_copy(
            hsend.at[tz], hrecv.at[z], gz_s, gz_r, device_id={"z": tz}, device_id_type=MESH
        ).start()

    each(1, NZ, scatter_z)
    hrecv[z] = hsend[z]
    out_copy.wait()
    wait_all(hrecv.at[pl.ds(0, NZ - 1)], gz_s, gz_r)
    whole = hrecv[0]
    for i in range(1, NZ):
        whole = whole + hrecv[i]
    grad_ref[...] = whole.astype(BF16)


def hand_over(loss_in, grad_in, fresh_in, loss_out, grad_out, fresh_out, loss, grad, fresh, sems):
    parts = 2
    size = ROWS // parts
    moves = [(loss_in, loss, loss_out), (grad_in, grad, grad_out)]
    for i in range(parts):
        at = pl.ds(i * size, size)
        moves.append((fresh_in.at[at], fresh.at[at], fresh_out.at[at]))
    ins = [pltpu.make_async_copy(a, b, sems.at[0, i]) for i, (a, b, _) in enumerate(moves)]
    outs = [pltpu.make_async_copy(b, c, sems.at[1, i]) for i, (_, b, c) in enumerate(moves)]
    for copy in ins:
        copy.start()
    for i in range(len(moves)):
        ins[i].wait()
        outs[i].start()
    for copy in outs:
        copy.wait()


def per_device(
    queries,
    positives,
    label_vectors,
    refresh_slot,
    features,
    encoder_weight,
    encoder_gain,
    free_vectors,
    targets,
):
    vmem = pl.BlockSpec(memory_space=pltpu.VMEM)
    hbm = pl.BlockSpec(memory_space=pl.ANY)
    dma = pltpu.SemaphoreType.DMA
    results = (
        jax.ShapeDtypeStruct((1, 2), F32),
        jax.ShapeDtypeStruct((2, D), BF16),
        jax.ShapeDtypeStruct((ROWS, D), BF16),
    )
    made = pl.pallas_call(
        kernel,
        out_shape=results,
        in_specs=[hbm] * 9,
        out_specs=(vmem, vmem, hbm),
        scratch_shapes=[
            pltpu.SMEM((1,), I32),
            pltpu.VMEM((2, POS, NQ), I32),
            pltpu.VMEM((ROWS, D), BF16),
            pltpu.VMEM((D, D), BF16),
            pltpu.VMEM((TILES, LANES), F32),
            pltpu.VMEM((2 * NCLS * 3, LANES), I32),
            pltpu.VMEM((NPLANE, NZ, 2, D), BF16),
            pltpu.VMEM((NQ, D), BF16),
            pltpu.VMEM((SLOTS, SLOT_ROWS, D), BF16),
            pltpu.VMEM((ROWS, D), BF16),
            pltpu.VMEM((2 * ROWS, HALF), BF16),
            pltpu.VMEM((NCLS, 2, 3 * HALF), BF16),
            pltpu.VMEM((NCLS, 2, 3 * HALF), BF16),
            pltpu.VMEM((2, ROWS, 3 * 2 * NCLS), BF16),
            pltpu.VMEM((2, ROWS, D), BF16),
            pltpu.VMEM((POS, NQ, LANES), I32),
            pltpu.VMEM((NQ, LANES), F32),
            pltpu.VMEM((SLOTS, NQ, SLOT_ROWS), F32),
            pltpu.VMEM((SLOTS, NQ, SLOT_ROWS), BF16),
            pltpu.VMEM((NQ, LANES), F32),
            pltpu.VMEM((NQ, LANES), F32),
            pltpu.VMEM((NQ, LANES), F32),
            pltpu.VMEM((NQ, LANES), F32),
            pltpu.VMEM((NQ, LANES), F32),
            pltpu.VMEM((SLOTS, 2 * NQ, SLOT_ROWS), BF16),
            pltpu.VMEM((2 * NQ, D), F32),
            pltpu.VMEM((NQ, D), F32),
            pltpu.VMEM((NQ, D), F32),
            pltpu.VMEM((NQ, D), F32),
            pltpu.VMEM((NPLANE, 2 * NZ, D), BF16),
            pltpu.VMEM((NPLANE, 2 * NZ, D), BF16),
            pltpu.VMEM((NZ, 2, D), F32),
            pltpu.VMEM((NZ, 2, D), F32),
            pltpu.VMEM((NPLANE, 4, NQ), F32),
            pltpu.VMEM((NZ, 4, NQ), F32),
            pltpu.SemaphoreType.REGULAR,
        ]
        + [dma] * 6
        + [dma((4,))]
        + [dma] * 6
        + [dma((2,))] * 2
        + [dma] * 8,
        compiler_params=pltpu.CompilerParams(
            collective_id=0, has_side_effects=True, vmem_limit_bytes=56 * 2**20
        ),
    )(
        refresh_slot.reshape(1),
        queries.reshape(2, D),
        jnp.swapaxes(positives, 1, 2),
        label_vectors.reshape(SLOTS, SLOT_ROWS, D),
        features,
        encoder_weight,
        encoder_gain.reshape(TILES, LANES),
        free_vectors,
        targets.reshape(-1, LANES),
    )
    loss, grads, refreshed = pl.pallas_call(
        hand_over,
        out_shape=results,
        in_specs=[hbm] * 3,
        out_specs=(hbm,) * 3,
        scratch_shapes=[
            pltpu.VMEM((1, 2), F32),
            pltpu.VMEM((2, D), BF16),
            pltpu.VMEM((ROWS, D), BF16),
            dma((2, 4)),
        ],
    )(*made)
    return loss, grads.reshape(1, 2, D), refreshed


def solution(mesh):
    torus = Mesh(mesh.devices.reshape(NY, NZ, NX, mesh.shape["rep"]), CLS_REP)
    placed = (
        P("core", CLS, None),
        P(),
        P(CLS, None),
        P(),
        P(CLS_REP, None),
        P(),
        P(),
        P(CLS_REP, None),
        P(),
    )
    return jax.shard_map(
        per_device,
        mesh=torus,
        in_specs=placed,
        out_specs=(P("core", CLS), P("core", CLS, None), P(CLS_REP, None)),
        check_vma=False,
    )
```

```python
import jax
import jax.numpy as jnp
from jax import lax
from jax.experimental import pallas as pl
from jax.experimental.pallas import tpu as pltpu
from jax.sharding import Mesh
from jax.sharding import PartitionSpec as P

F32 = jnp.float32
BF16 = jnp.bfloat16
I32 = jnp.int32
MESH = pl.DeviceIdType.MESH
CLS = ("y", "z", "x")
CLS_REP = ("y", "z", "x", "core")
NY, NZ, NX = 4, 8, 4
NPLANE = NX * NY
NCLS = NPLANE * NZ
D = 768
HALF = D // 2
ROWS = 384
SLOTS = 8
SLOT_ROWS = 768
LABELS_DEV = SLOTS * SLOT_ROWS
NQ = 256
POS = 4
CHUNK = 32
LANES = 128
TILES = SLOT_ROWS // LANES
EARLY = 1
UNDER_SWAP = 1
FIRST = 1
MIDDLE = 5


def dot(a, b):
    return jnp.dot(a, b, preferred_element_type=F32)


def dot_t(a, b):
    return lax.dot_general(a, b, (((1,), (1,)), ((), ())), preferred_element_type=F32)


def each(lo, hi, fn):
    def step(k, carry):
        fn(k)
        return carry

    lax.fori_loop(lo, hi, step, 0)


def three_of(parts, inside):
    low = high = total = None
    for part, mask in zip(parts, inside):
        lo = jnp.min(jnp.where(mask, part, 1e9), axis=1, keepdims=True)
        hi = jnp.max(jnp.where(mask, part, -1.0), axis=1, keepdims=True)
        su = jnp.sum(jnp.where(mask, part, 0.0), axis=1, keepdims=True)
        low = lo if low is None else jnp.minimum(low, lo)
        high = hi if high is None else jnp.maximum(high, hi)
        total = su if total is None else total + su
    return low, total - low - high, high


def merged(stats, count):
    peak = stats[0, 0:1, :]
    for i in range(1, count):
        peak = jnp.maximum(peak, stats[i, 0:1, :])
    total = jnp.zeros_like(peak)
    positive = jnp.zeros_like(peak)
    for i in range(count):
        total = total + stats[i, 1:2, :] * jnp.exp(stats[i, 0:1, :] - peak)
        positive = positive + stats[i, 2:3, :]
    return peak, total, positive


def kernel(
    slot_hbm, q_hbm, pos_hbm, lab_hbm, feat_hbm, w_hbm, gain_hbm, free_hbm, tgt_hbm,
    loss_ref, grad_ref, fresh_hbm,
    slot_ref, pos_ref, feat_ref, w_ref, gain_ref, tgt_ref,
    qg, qm, lab, free, enc2, send, recv, put, fresh, off, inv, lg, cnt, mx, top_ref, sacc, pacc, ltb, coef, gacc, gcnt, gu, gt,
    gsend, grecv, hsend, hrecv, st_p, st_z,
    ready,
    lab_sem, free_sem, q_sem, out_sem, w_sem, feat_sem, small_sem,
    qz_s, qz_r, qp_s, qp_r, d_s, d_r, f_s, f_r, sp_s, sp_r, sz_s, sz_r, gp_s, gp_r, gz_s, gz_r,
):
    y, z, x = lax.axis_index("y"), lax.axis_index("z"), lax.axis_index("x")
    core = lax.axis_index("core")
    me = (y * NZ + z) * NX + x
    plane = x * NY + y

    def z_peer(k):
        return lax.rem(z + k, NZ)

    def plane_peer(k):
        return lax.rem(x + lax.div(k, NY), NX), lax.rem(y + lax.rem(k, NY), NY)

    sent = []

    def wait_all(ref, s, r):
        pltpu.make_async_copy(ref, ref, r).wait()
        sent.append((ref, s))

    barrier = pltpu.get_barrier_semaphore()

    def greet_z(k):
        pl.semaphore_signal(barrier, inc=1, device_id={"z": z_peer(k)}, device_id_type=MESH)

    def greet_plane(k):
        tx, ty = plane_peer(k)
        pl.semaphore_signal(barrier, inc=1, device_id={"x": tx, "y": ty}, device_id_type=MESH)

    each(1, NZ, greet_z)
    each(1, NPLANE, greet_plane)
    pl.semaphore_signal(barrier, inc=1, device_id={"core": 1 - core}, device_id_type=MESH)

    q_copy = pltpu.make_async_copy(q_hbm, qg.at[plane, z], q_sem)
    w_copy = pltpu.make_async_copy(w_hbm, w_ref, w_sem)
    feat_copy = pltpu.make_async_copy(feat_hbm, feat_ref, feat_sem)
    gain_copy = pltpu.make_async_copy(gain_hbm, gain_ref, small_sem.at[0])
    pos_copy = pltpu.make_async_copy(pos_hbm, pos_ref, small_sem.at[1])
    tgt_copy = pltpu.make_async_copy(tgt_hbm, tgt_ref, small_sem.at[2])
    free_copy = pltpu.make_async_copy(free_hbm, free, free_sem)
    lab_copy = pltpu.make_async_copy(lab_hbm, lab, lab_sem)
    slot_copy = pltpu.make_async_copy(slot_hbm, slot_ref, small_sem.at[3])
    for copy in (w_copy, feat_copy, gain_copy, tgt_copy, q_copy, pos_copy, slot_copy, free_copy, lab_copy):
        copy.start()

    w_copy.wait()
    feat_copy.wait()
    gain_copy.wait()
    hidden = dot(feat_ref[...], w_ref[...])
    scale = lax.rsqrt(jnp.mean(hidden * hidden, axis=1, keepdims=True) + 1e-06)
    for c in range(2):
        for j in range(TILES // 2):
            i = c * (TILES // 2) + j
            cols = hidden[:, i * LANES : (i + 1) * LANES] * scale * gain_ref[i : i + 1, :]
            enc2[c * ROWS : (c + 1) * ROWS, j * LANES : (j + 1) * LANES] = cols.astype(BF16)

    tgt_copy.wait()
    block = me * 2 + core
    row = lax.broadcasted_iota(I32, (2 * NCLS, LANES), 0)
    owner_base = (row // 2) * SLOT_ROWS
    parts = []
    inside = []
    for k in range(3):
        part = tgt_ref[pl.ds(3 * block + k, 1), :] - owner_base
        parts.append(part.astype(F32))
        inside.append((part >= 0) & (part < SLOT_ROWS))
    picks = three_of(parts, inside)
    even = row % 2 == 0
    for r in range(3):
        hit = [part == picks[r] for part in parts]
        one = [jnp.where(h & even, 1.0, 0.0).astype(BF16) for h in hit]
        two = [jnp.where(h & ~even, 1.0, 0.0).astype(BF16) for h in hit]
        chosen = dot(jnp.concatenate(one + two, axis=1), enc2[...])
        send[:, :, r * HALF : (r + 1) * HALF] = chosen.astype(BF16).reshape(NCLS, 2, HALF)

    q_copy.wait()
    pl.semaphore_wait(barrier, NZ - 1 + NPLANE - 1 + 1)

    def ready_z(k):
        pl.semaphore_signal(ready, inc=1, device_id={"z": z_peer(k)}, device_id_type=MESH)

    def gather_z(k):
        pltpu.make_async_remote_copy(
            qg.at[plane, z], qg.at[plane, z], qz_s, qz_r, device_id={"z": z_peer(k)}, device_id_type=MESH
        ).start()

    each(1, NZ, ready_z)
    each(1, NZ, gather_z)

    def gather_plane(k):
        tx, ty = plane_peer(k)
        pltpu.make_async_remote_copy(
            qg.at[plane], qg.at[plane], qp_s, qp_r, device_id={"x": tx, "y": ty}, device_id_type=MESH
        ).start()

    def dispatch(dz, j):
        tz = z_peer(dz)
        tx, ty = plane_peer(j)
        dest = (ty * NZ + tz) * NX + tx
        pltpu.make_async_remote_copy(
            send.at[dest], recv.at[me], d_s, d_r, device_id={"y": ty, "z": tz, "x": tx}, device_id_type=MESH
        ).start()

    def dispatch_far(j):
        tx, ty = plane_peer(j)
        for dz in range(1, NZ):
            tz = z_peer(dz)
            dest = (ty * NZ + tz) * NX + tx
            pltpu.make_async_remote_copy(
                send.at[dest], recv.at[me], d_s, d_r, device_id={"y": ty, "z": tz, "x": tx}, device_id_type=MESH
            ).start()


    parts = []
    inside = []
    for k in range(3):
        first = tgt_ref[pl.ds(k, NCLS, stride=6), :]
        second = tgt_ref[pl.ds(3 + k, NCLS, stride=6), :]
        part = jnp.where(core == 0, first, second) - (me * SLOT_ROWS + core * ROWS)
        parts.append(part.astype(F32))
        inside.append((part >= 0) & (part < ROWS))
    picks = three_of(parts, inside)
    lane = lax.broadcasted_iota(I32, (NCLS, ROWS), 1).astype(F32)
    spread_row = lax.broadcasted_iota(I32, (NCLS, 2 * NCLS), 0) * 2
    spread_col = lax.broadcasted_iota(I32, (NCLS, 2 * NCLS), 1)
    for r in range(3):
        to_row = jnp.where(lane == picks[r], 1.0, 0.0).T.astype(BF16)
        for c in range(2):
            spread = jnp.where(spread_col == spread_row + c, 1.0, 0.0).astype(BF16)
            put[c, :, r * 2 * NCLS : (r + 1) * 2 * NCLS] = dot(to_row, spread).astype(BF16)

    pos_copy.wait()
    slot_copy.wait()
    slot = slot_ref[0]
    q_row = lax.broadcasted_iota(I32, (NQ, NQ), 0)
    q_col = lax.broadcasted_iota(I32, (NQ, NQ), 1)
    natural = ((((q_row // 16) % NY) * NZ + (q_row // 2) % NZ) * NX + q_row // 64) * 2 + q_row % 2
    order = jnp.where(q_col == natural, 1.0, 0.0).astype(BF16)
    ids = pos_ref[core] + 1
    ids = sum(
        dot_t(order, ((ids >> (8 * i)) & 255).astype(F32).astype(BF16)) * float(256**i) for i in range(3)
    )
    valid = ids >= 1.0
    count = jnp.sum(jnp.where(valid, 1.0, 0.0), axis=1, keepdims=True)
    inv[...] = jnp.broadcast_to(1.0 / count, (NQ, LANES))
    local = jnp.where(valid, ids.astype(I32) - (1 + me * LABELS_DEV), -LABELS_DEV)
    for j in range(POS):
        off[j] = jnp.broadcast_to(local[:, j : j + 1], (NQ, LANES))

    def slot_of(k):
        return lax.rem(slot + 1 + k, SLOTS)

    nblocks = NQ // CHUNK

    def counts(k):
        base = slot_of(k) * SLOT_ROWS

        def rows(b):
            at = pl.ds(b * CHUNK, CHUNK)
            lane_id = lax.broadcasted_iota(I32, (CHUNK, LANES), 1) + base
            offs = [off[j, at, :] - lane_id for j in range(POS)]
            for c in range(TILES):
                acc = jnp.zeros((CHUNK, LANES), F32)
                for j in range(POS):
                    acc = acc + jnp.where(offs[j] == c * LANES, 1.0, 0.0)
                cnt[k, at, c * LANES : (c + 1) * LANES] = acc.astype(BF16)

        each(0, nblocks, rows)

    each(0, SLOTS, counts)

    pl.semaphore_wait(ready, NZ - 1)
    each(1, FIRST, dispatch_far)
    wait_all(qg.at[plane, pl.ds(0, NZ - 1)], qz_s, qz_r)
    each(1, NPLANE, gather_plane)
    each(1, NZ, lambda k: dispatch(k, 0))
    each(1, NPLANE, lambda j: dispatch(0, j))
    each(FIRST, NPLANE, dispatch_far)
    recv[me] = send[me]

    lab_copy.wait()
    gcnt[...] = dot(cnt[0], lab[slot_of(0)])

    def count_rows(k):
        gcnt[...] += dot(cnt[k], lab[slot_of(k)])

    each(1, SLOTS - 1, count_rows)
    wait_all(qg.at[pl.ds(0, NPLANE - 1)], qp_s, qp_r)
    qm[...] = qg[...].reshape(NQ, D)

    def highest(values):
        top = values[:, 0:LANES]
        for c in range(1, values.shape[1] // LANES):
            top = jnp.maximum(top, values[:, c * LANES : (c + 1) * LANES])
        return top

    def logits_of(k, peak):
        values = dot_t(qm[...], lab[slot_of(k)])
        lg[k] = values
        return jnp.maximum(peak, highest(values))

    peak = lax.fori_loop(0, SLOTS - 1, logits_of, jnp.full((NQ, LANES), -jnp.inf, F32))
    mx[...] = jnp.broadcast_to(jnp.max(peak, axis=1, keepdims=True), (NQ, LANES))
    sacc[...] = jnp.zeros((NQ, LANES), F32)
    positive = jnp.zeros((NQ, LANES), F32)
    for c in range(TILES):
        cols = slice(c * LANES, (c + 1) * LANES)
        positive = positive + qm[:, cols].astype(F32) * gcnt[:, cols]
    pacc[...] = positive

    def weights(k, level_ref):
        def rows(b):
            at = pl.ds(b * CHUNK, CHUNK)
            low_at = pl.ds(NQ + b * CHUNK, CHUNK)
            level = level_ref[at, :]
            s = sacc[at, :]
            for c in range(TILES):
                cols = slice(c * LANES, (c + 1) * LANES)
                e = jnp.exp(lg[k, at, cols] - level)
                s = s + e
                high = e.astype(BF16)
                coef[k, at, cols] = high
                coef[k, low_at, cols] = (e - high.astype(F32)).astype(BF16)
            sacc[at, :] = s

        each(0, nblocks, rows)

    each(0, SLOTS - 1, lambda k: weights(k, mx))

    def gradients(k):
        gacc[...] += dot(coef[k], lab[slot_of(k)])

    each(1, EARLY, gradients)

    free_copy.wait()
    wait_all(recv.at[pl.ds(0, NCLS - 1)], d_s, d_r)
    arrived = recv[...].reshape(2 * NCLS, 3 * HALF)
    stacked = jnp.concatenate([arrived[:, r * HALF : (r + 1) * HALF] for r in range(3)], axis=0)
    swaps = []
    for h in range(2):
        at = slice(h * (ROWS // 2), (h + 1) * (ROWS // 2))
        for c in range(2):
            cols = slice(c * HALF, (c + 1) * HALF)
            fresh[core, at, cols] = (free[at, cols].astype(F32) + dot(put[c, at, :], stacked)).astype(BF16)
        swap = pltpu.make_async_remote_copy(
            fresh.at[core, at], fresh.at[core, at], f_s.at[h], f_r.at[h],
            device_id={"core": 1 - core}, device_id_type=MESH,
        )
        swap.start()
        swaps.append(swap)
    out_copy = pltpu.make_async_copy(fresh.at[core], fresh_hbm, out_sem)
    out_copy.start()
    own_logits = dot_t(qm[...], fresh[core])
    each(EARLY, UNDER_SWAP, gradients)
    for h, swap in enumerate(swaps):
        swap.wait_recv()
        sent.append((fresh.at[0, pl.ds(0, ROWS // 2)], f_s.at[h]))
    other_logits = dot_t(qm[...], fresh[1 - core])
    peak = jnp.maximum(highest(own_logits), highest(other_logits))
    lg[SLOTS - 1, :, 0:ROWS] = jnp.where(core == 0, own_logits, other_logits)
    lg[SLOTS - 1, :, ROWS : 2 * ROWS] = jnp.where(core == 0, other_logits, own_logits)
    old = mx[...]
    top = jnp.maximum(old, jnp.broadcast_to(jnp.max(peak, axis=1, keepdims=True), (NQ, LANES)))
    sacc[...] = sacc[...] * jnp.exp(old - top)
    top_ref[...] = top
    weights(SLOTS - 1, top_ref)
    positive = pacc[...]
    for c in range(TILES):
        cols = slice(c * LANES, (c + 1) * LANES)
        positive = positive + cnt[SLOTS - 1, :, cols].astype(F32) * lg[SLOTS - 1, :, cols]
    pacc[...] = positive

    st_p[plane, 0:1, :] = top_ref[...].T[0:1, :]
    st_p[plane, 1:2, :] = jnp.sum(sacc[...].T, axis=0, keepdims=True)
    st_p[plane, 2:3, :] = jnp.sum((pacc[...] * inv[...]).T, axis=0, keepdims=True)
    st_p[plane, 3:4, :] = jnp.zeros((1, NQ), F32)

    def stats_plane(k):
        tx, ty = plane_peer(k)
        pltpu.make_async_remote_copy(
            st_p.at[plane], st_p.at[plane], sp_s, sp_r, device_id={"x": tx, "y": ty}, device_id_type=MESH
        ).start()

    each(1, NPLANE, stats_plane)
    gacc[...] = dot(coef[0], lab[slot_of(0)])
    each(UNDER_SWAP, MIDDLE, gradients)
    wait_all(st_p.at[pl.ds(0, NPLANE - 1)], sp_s, sp_r)
    peak, total, positive = merged(st_p, NPLANE)
    st_z[z, 0:1, :] = peak
    st_z[z, 1:2, :] = total
    st_z[z, 2:3, :] = positive
    st_z[z, 3:4, :] = jnp.zeros((1, NQ), F32)

    def stats_z(k):
        pltpu.make_async_remote_copy(
            st_z.at[z], st_z.at[z], sz_s, sz_r, device_id={"z": z_peer(k)}, device_id_type=MESH
        ).start()

    each(1, NZ, stats_z)
    each(MIDDLE, SLOTS - 1, gradients)
    new = fresh[...].reshape(SLOT_ROWS, D)
    last = dot(coef[SLOTS - 1], new)
    last_count = dot(cnt[SLOTS - 1], new)
    factor = jnp.exp(mx[...] - top_ref[...])
    for c in range(TILES):
        cols = slice(c * LANES, (c + 1) * LANES)
        gu[:, cols] = (gacc[0:NQ, cols] + gacc[NQ : 2 * NQ, cols]) * factor + (last[0:NQ, cols] + last[NQ : 2 * NQ, cols])
        gt[:, cols] = (gcnt[:, cols] + last_count[:, cols]) * inv[...]
    wait_all(st_z.at[pl.ds(0, NZ - 1)], sz_s, sz_r)
    peak, total, positive = merged(st_z, NZ)
    log_total = peak + jnp.log(total)
    ltb[...] = jnp.exp(top_ref[...] - jnp.broadcast_to(log_total, (LANES, NQ)).T)
    for c in range(TILES):
        cols = slice(c * LANES, (c + 1) * LANES)
        gsend[:, :, cols] = (gu[:, cols] * ltb[...] - gt[:, cols]).astype(BF16).reshape(NPLANE, 2 * NZ, LANES)

    def scatter_plane(k):
        tx, ty = plane_peer(k)
        pltpu.make_async_remote_copy(
            gsend.at[tx * NY + ty], grecv.at[plane], gp_s, gp_r, device_id={"x": tx, "y": ty}, device_id_type=MESH
        ).start()

    each(1, NPLANE, scatter_plane)
    grecv[plane] = gsend[plane]
    loss = log_total - positive
    own = (plane * NZ + z) * 2
    query = lax.broadcasted_iota(I32, (1, NQ), 1)
    for i in range(2):
        loss_ref[:, i : i + 1] = jnp.sum(jnp.where(query == own + i, loss, 0.0), axis=1, keepdims=True)
    wait_all(grecv.at[pl.ds(0, NPLANE - 1)], gp_s, gp_r)
    part = grecv[0].astype(F32)
    for i in range(1, NPLANE):
        part = part + grecv[i].astype(F32)
    hsend[...] = part.reshape(NZ, 2, D)

    def scatter_z(k):
        tz = z_peer(k)
        pltpu.make_async_remote_copy(
            hsend.at[tz], hrecv.at[z], gz_s, gz_r, device_id={"z": tz}, device_id_type=MESH
        ).start()

    each(1, NZ, scatter_z)
    hrecv[z] = hsend[z]
    out_copy.wait()
    wait_all(hrecv.at[pl.ds(0, NZ - 1)], gz_s, gz_r)
    whole = hrecv[0]
    for i in range(1, NZ):
        whole = whole + hrecv[i]
    grad_ref[...] = whole.astype(BF16)
    for ref, s in sent:
        pltpu.make_async_copy(ref, ref, s).wait()


def hand_over(loss_in, grad_in, fresh_in, loss_out, grad_out, fresh_out, loss, grad, fresh, sems):
    parts = 2
    size = ROWS // parts
    moves = [(loss_in, loss, loss_out), (grad_in, grad, grad_out)]
    for i in range(parts):
        at = pl.ds(i * size, size)
        moves.append((fresh_in.at[at], fresh.at[at], fresh_out.at[at]))
    ins = [pltpu.make_async_copy(a, b, sems.at[0, i]) for i, (a, b, _) in enumerate(moves)]
    outs = [pltpu.make_async_copy(b, c, sems.at[1, i]) for i, (_, b, c) in enumerate(moves)]
    for copy in ins:
        copy.start()
    for i in range(len(moves)):
        ins[i].wait()
        outs[i].start()
    for copy in outs:
        copy.wait()


def per_device(
    queries,
    positives,
    label_vectors,
    refresh_slot,
    features,
    encoder_weight,
    encoder_gain,
    free_vectors,
    targets,
):
    vmem = pl.BlockSpec(memory_space=pltpu.VMEM)
    hbm = pl.BlockSpec(memory_space=pl.ANY)
    dma = pltpu.SemaphoreType.DMA
    results = (
        jax.ShapeDtypeStruct((1, 2), F32),
        jax.ShapeDtypeStruct((2, D), BF16),
        jax.ShapeDtypeStruct((ROWS, D), BF16),
    )
    made = pl.pallas_call(
        kernel,
        out_shape=results,
        in_specs=[hbm] * 9,
        out_specs=(vmem, vmem, hbm),
        scratch_shapes=[
            pltpu.SMEM((1,), I32),
            pltpu.VMEM((2, POS, NQ), I32),
            pltpu.VMEM((ROWS, D), BF16),
            pltpu.VMEM((D, D), BF16),
            pltpu.VMEM((TILES, LANES), F32),
            pltpu.VMEM((2 * NCLS * 3, LANES), I32),
            pltpu.VMEM((NPLANE, NZ, 2, D), BF16),
            pltpu.VMEM((NQ, D), BF16),
            pltpu.VMEM((SLOTS, SLOT_ROWS, D), BF16),
            pltpu.VMEM((ROWS, D), BF16),
            pltpu.VMEM((2 * ROWS, HALF), BF16),
            pltpu.VMEM((NCLS, 2, 3 * HALF), BF16),
            pltpu.VMEM((NCLS, 2, 3 * HALF), BF16),
            pltpu.VMEM((2, ROWS, 3 * 2 * NCLS), BF16),
            pltpu.VMEM((2, ROWS, D), BF16),
            pltpu.VMEM((POS, NQ, LANES), I32),
            pltpu.VMEM((NQ, LANES), F32),
            pltpu.VMEM((SLOTS, NQ, SLOT_ROWS), F32),
            pltpu.VMEM((SLOTS, NQ, SLOT_ROWS), BF16),
            pltpu.VMEM((NQ, LANES), F32),
            pltpu.VMEM((NQ, LANES), F32),
            pltpu.VMEM((NQ, LANES), F32),
            pltpu.VMEM((NQ, LANES), F32),
            pltpu.VMEM((NQ, LANES), F32),
            pltpu.VMEM((SLOTS, 2 * NQ, SLOT_ROWS), BF16),
            pltpu.VMEM((2 * NQ, D), F32),
            pltpu.VMEM((NQ, D), F32),
            pltpu.VMEM((NQ, D), F32),
            pltpu.VMEM((NQ, D), F32),
            pltpu.VMEM((NPLANE, 2 * NZ, D), BF16),
            pltpu.VMEM((NPLANE, 2 * NZ, D), BF16),
            pltpu.VMEM((NZ, 2, D), F32),
            pltpu.VMEM((NZ, 2, D), F32),
            pltpu.VMEM((NPLANE, 4, NQ), F32),
            pltpu.VMEM((NZ, 4, NQ), F32),
            pltpu.SemaphoreType.REGULAR,
        ]
        + [dma] * 6
        + [dma((4,))]
        + [dma] * 6
        + [dma((2,))] * 2
        + [dma] * 8,
        compiler_params=pltpu.CompilerParams(
            collective_id=0, has_side_effects=True, vmem_limit_bytes=56 * 2**20
        ),
    )(
        refresh_slot.reshape(1),
        queries.reshape(2, D),
        jnp.swapaxes(positives, 1, 2),
        label_vectors.reshape(SLOTS, SLOT_ROWS, D),
        features,
        encoder_weight,
        encoder_gain.reshape(TILES, LANES),
        free_vectors,
        targets.reshape(-1, LANES),
    )
    loss, grads, refreshed = pl.pallas_call(
        hand_over,
        out_shape=results,
        in_specs=[hbm] * 3,
        out_specs=(hbm,) * 3,
        scratch_shapes=[
            pltpu.VMEM((1, 2), F32),
            pltpu.VMEM((2, D), BF16),
            pltpu.VMEM((ROWS, D), BF16),
            dma((2, 4)),
        ],
    )(*made)
    return loss, grads.reshape(1, 2, D), refreshed


def solution(mesh):
    torus = Mesh(mesh.devices.reshape(NY, NZ, NX, mesh.shape["rep"]), CLS_REP)
    placed = (
        P("core", CLS, None),
        P(),
        P(CLS, None),
        P(),
        P(CLS_REP, None),
        P(),
        P(),
        P(CLS_REP, None),
        P(),
    )
    return jax.shard_map(
        per_device,
        mesh=torus,
        in_specs=placed,
        out_specs=(P("core", CLS), P("core", CLS, None), P(CLS_REP, None)),
        check_vma=False,
    )
```

```python
import jax
import jax.numpy as jnp
from jax import lax
from jax.experimental import pallas as pl
from jax.experimental.pallas import tpu as pltpu
from jax.sharding import Mesh
from jax.sharding import PartitionSpec as P

F32 = jnp.float32
BF16 = jnp.bfloat16
I32 = jnp.int32
MESH = pl.DeviceIdType.MESH
CLS = ("y", "z", "x")
CLS_REP = ("y", "z", "x", "core")
NY, NZ, NX = 4, 8, 4
NPLANE = NX * NY
NCLS = NPLANE * NZ
D = 768
HALF = D // 2
ROWS = 384
SLOTS = 8
SLOT_ROWS = 768
LABELS_DEV = SLOTS * SLOT_ROWS
NQ = 256
POS = 4
CHUNK = 32
LANES = 128
TILES = SLOT_ROWS // LANES
FIRST = 1
MIDDLE = 5


def dot(a, b):
    return jnp.dot(a, b, preferred_element_type=F32)


def dot_t(a, b):
    return lax.dot_general(a, b, (((1,), (1,)), ((), ())), preferred_element_type=F32)


def each(lo, hi, fn):
    def step(k, carry):
        fn(k)
        return carry

    lax.fori_loop(lo, hi, step, 0)


def three_of(parts, inside):
    low = high = total = None
    for part, mask in zip(parts, inside):
        lo = jnp.min(jnp.where(mask, part, 1e9), axis=1, keepdims=True)
        hi = jnp.max(jnp.where(mask, part, -1.0), axis=1, keepdims=True)
        su = jnp.sum(jnp.where(mask, part, 0.0), axis=1, keepdims=True)
        low = lo if low is None else jnp.minimum(low, lo)
        high = hi if high is None else jnp.maximum(high, hi)
        total = su if total is None else total + su
    return low, total - low - high, high


def merged(stats, count):
    peak = stats[0, 0:1, :]
    for i in range(1, count):
        peak = jnp.maximum(peak, stats[i, 0:1, :])
    total = jnp.zeros_like(peak)
    positive = jnp.zeros_like(peak)
    for i in range(count):
        total = total + stats[i, 1:2, :] * jnp.exp(stats[i, 0:1, :] - peak)
        positive = positive + stats[i, 2:3, :]
    return peak, total, positive


def kernel(
    slot_hbm, q_hbm, pos_hbm, lab_hbm, feat_hbm, w_hbm, gain_hbm, free_hbm, tgt_hbm,
    loss_ref, grad_ref, fresh_hbm,
    slot_ref, pos_ref, feat_ref, w_ref, gain_ref, tgt_ref,
    qg, qm, lab, free, enc2, send, recv, put, fresh, off, inv, lg, cnt, mx, top_ref, sacc, pacc, ltb, coef, gacc, gcnt, gu, gt,
    gsend, grecv, hsend, hrecv, st_p, st_z,
    ready,
    lab_sem, free_sem, q_sem, out_sem, w_sem, feat_sem, small_sem,
    qz_s, qz_r, qp_s, qp_r, d_s, d_r, f_s, f_r, sp_s, sp_r, sz_s, sz_r, gp_s, gp_r, gz_s, gz_r,
):
    y, z, x = lax.axis_index("y"), lax.axis_index("z"), lax.axis_index("x")
    core = lax.axis_index("core")
    me = (y * NZ + z) * NX + x
    plane = x * NY + y

    def z_peer(k):
        return lax.rem(z + k, NZ)

    def plane_peer(k):
        return lax.rem(x + lax.div(k, NY), NX), lax.rem(y + lax.rem(k, NY), NY)

    sent = []

    def wait_all(ref, s, r):
        pltpu.make_async_copy(ref, ref, r).wait()
        sent.append((ref, s))

    barrier = pltpu.get_barrier_semaphore()

    def greet_z(k):
        pl.semaphore_signal(barrier, inc=1, device_id={"z": z_peer(k)}, device_id_type=MESH)

    def greet_plane(k):
        tx, ty = plane_peer(k)
        pl.semaphore_signal(barrier, inc=1, device_id={"x": tx, "y": ty}, device_id_type=MESH)

    each(1, NZ, greet_z)
    each(1, NPLANE, greet_plane)
    pl.semaphore_signal(barrier, inc=1, device_id={"core": 1 - core}, device_id_type=MESH)

    q_copy = pltpu.make_async_copy(q_hbm, qg.at[plane, z], q_sem)
    w_copy = pltpu.make_async_copy(w_hbm, w_ref, w_sem)
    feat_copy = pltpu.make_async_copy(feat_hbm, feat_ref, feat_sem)
    gain_copy = pltpu.make_async_copy(gain_hbm, gain_ref, small_sem.at[0])
    pos_copy = pltpu.make_async_copy(pos_hbm, pos_ref, small_sem.at[1])
    tgt_copy = pltpu.make_async_copy(tgt_hbm, tgt_ref, small_sem.at[2])
    free_copy = pltpu.make_async_copy(free_hbm, free, free_sem)
    lab_copy = pltpu.make_async_copy(lab_hbm, lab, lab_sem)
    slot_copy = pltpu.make_async_copy(slot_hbm, slot_ref, small_sem.at[3])
    for copy in (w_copy, feat_copy, gain_copy, tgt_copy, q_copy, pos_copy, slot_copy, free_copy, lab_copy):
        copy.start()

    w_copy.wait()
    feat_copy.wait()
    gain_copy.wait()
    hidden = dot(feat_ref[...], w_ref[...])
    scale = lax.rsqrt(jnp.mean(hidden * hidden, axis=1, keepdims=True) + 1e-06)
    for c in range(2):
        for j in range(TILES // 2):
            i = c * (TILES // 2) + j
            cols = hidden[:, i * LANES : (i + 1) * LANES] * scale * gain_ref[i : i + 1, :]
            enc2[c * ROWS : (c + 1) * ROWS, j * LANES : (j + 1) * LANES] = cols.astype(BF16)

    tgt_copy.wait()
    block = me * 2 + core
    row = lax.broadcasted_iota(I32, (2 * NCLS, LANES), 0)
    owner_base = (row // 2) * SLOT_ROWS
    parts = []
    inside = []
    for k in range(3):
        part = tgt_ref[pl.ds(3 * block + k, 1), :] - owner_base
        parts.append(part.astype(F32))
        inside.append((part >= 0) & (part < SLOT_ROWS))
    picks = three_of(parts, inside)
    even = row % 2 == 0
    for r in range(3):
        hit = [part == picks[r] for part in parts]
        one = [jnp.where(h & even, 1.0, 0.0).astype(BF16) for h in hit]
        two = [jnp.where(h & ~even, 1.0, 0.0).astype(BF16) for h in hit]
        chosen = dot(jnp.concatenate(one + two, axis=1), enc2[...])
        send[:, :, r * HALF : (r + 1) * HALF] = chosen.astype(BF16).reshape(NCLS, 2, HALF)

    q_copy.wait()
    pl.semaphore_wait(barrier, NZ - 1 + NPLANE - 1 + 1)

    def ready_z(k):
        pl.semaphore_signal(ready, inc=1, device_id={"z": z_peer(k)}, device_id_type=MESH)

    def gather_z(k):
        pltpu.make_async_remote_copy(
            qg.at[plane, z], qg.at[plane, z], qz_s, qz_r, device_id={"z": z_peer(k)}, device_id_type=MESH
        ).start()

    each(1, NZ, ready_z)
    each(1, NZ, gather_z)

    def gather_plane(k):
        tx, ty = plane_peer(k)
        pltpu.make_async_remote_copy(
            qg.at[plane], qg.at[plane], qp_s, qp_r, device_id={"x": tx, "y": ty}, device_id_type=MESH
        ).start()

    def dispatch(dz, j):
        tz = z_peer(dz)
        tx, ty = plane_peer(j)
        dest = (ty * NZ + tz) * NX + tx
        pltpu.make_async_remote_copy(
            send.at[dest], recv.at[me], d_s, d_r, device_id={"y": ty, "z": tz, "x": tx}, device_id_type=MESH
        ).start()

    def dispatch_far(j):
        tx, ty = plane_peer(j)
        for dz in range(1, NZ):
            tz = z_peer(dz)
            dest = (ty * NZ + tz) * NX + tx
            pltpu.make_async_remote_copy(
                send.at[dest], recv.at[me], d_s, d_r, device_id={"y": ty, "z": tz, "x": tx}, device_id_type=MESH
            ).start()


    parts = []
    inside = []
    for k in range(3):
        first = tgt_ref[pl.ds(k, NCLS, stride=6), :]
        second = tgt_ref[pl.ds(3 + k, NCLS, stride=6), :]
        part = jnp.where(core == 0, first, second) - (me * SLOT_ROWS + core * ROWS)
        parts.append(part.astype(F32))
        inside.append((part >= 0) & (part < ROWS))
    picks = three_of(parts, inside)
    lane = lax.broadcasted_iota(I32, (NCLS, ROWS), 1).astype(F32)
    spread_row = lax.broadcasted_iota(I32, (NCLS, 2 * NCLS), 0) * 2
    spread_col = lax.broadcasted_iota(I32, (NCLS, 2 * NCLS), 1)
    for r in range(3):
        to_row = jnp.where(lane == picks[r], 1.0, 0.0).T.astype(BF16)
        for c in range(2):
            spread = jnp.where(spread_col == spread_row + c, 1.0, 0.0).astype(BF16)
            put[c, :, r * 2 * NCLS : (r + 1) * 2 * NCLS] = dot(to_row, spread).astype(BF16)

    pos_copy.wait()
    slot_copy.wait()
    slot = slot_ref[0]
    q_row = lax.broadcasted_iota(I32, (NQ, NQ), 0)
    q_col = lax.broadcasted_iota(I32, (NQ, NQ), 1)
    natural = ((((q_row // 16) % NY) * NZ + (q_row // 2) % NZ) * NX + q_row // 64) * 2 + q_row % 2
    order = jnp.where(q_col == natural, 1.0, 0.0).astype(BF16)
    ids = pos_ref[core] + 1
    ids = sum(
        dot_t(order, ((ids >> (8 * i)) & 255).astype(F32).astype(BF16)) * float(256**i) for i in range(3)
    )
    valid = ids >= 1.0
    count = jnp.sum(jnp.where(valid, 1.0, 0.0), axis=1, keepdims=True)
    inv[...] = jnp.broadcast_to(1.0 / count, (NQ, LANES))
    local = jnp.where(valid, ids.astype(I32) - (1 + me * LABELS_DEV), -LABELS_DEV)
    for j in range(POS):
        off[j] = jnp.broadcast_to(local[:, j : j + 1], (NQ, LANES))

    def slot_of(k):
        return lax.rem(slot + 1 + k, SLOTS)

    nblocks = NQ // CHUNK

    def counts(k):
        base = slot_of(k) * SLOT_ROWS

        def rows(b):
            at = pl.ds(b * CHUNK, CHUNK)
            lane_id = lax.broadcasted_iota(I32, (CHUNK, LANES), 1) + base
            offs = [off[j, at, :] - lane_id for j in range(POS)]
            for c in range(TILES):
                acc = jnp.zeros((CHUNK, LANES), F32)
                for j in range(POS):
                    acc = acc + jnp.where(offs[j] == c * LANES, 1.0, 0.0)
                cnt[k, at, c * LANES : (c + 1) * LANES] = acc.astype(BF16)

        each(0, nblocks, rows)

    each(0, SLOTS, counts)

    pl.semaphore_wait(ready, NZ - 1)
    each(1, FIRST, dispatch_far)
    wait_all(qg.at[plane, pl.ds(0, NZ - 1)], qz_s, qz_r)
    each(1, NPLANE, gather_plane)
    each(1, NZ, lambda k: dispatch(k, 0))
    each(1, NPLANE, lambda j: dispatch(0, j))
    each(FIRST, NPLANE, dispatch_far)
    recv[me] = send[me]

    lab_copy.wait()
    gcnt[...] = dot(cnt[0], lab[slot_of(0)])

    def count_rows(k):
        gcnt[...] += dot(cnt[k], lab[slot_of(k)])

    each(1, SLOTS - 1, count_rows)
    wait_all(qg.at[pl.ds(0, NPLANE - 1)], qp_s, qp_r)
    qm[...] = qg[...].reshape(NQ, D)

    def highest(values):
        top = values[:, 0:LANES]
        for c in range(1, values.shape[1] // LANES):
            top = jnp.maximum(top, values[:, c * LANES : (c + 1) * LANES])
        return top

    def logits_of(k, peak):
        values = dot_t(qm[...], lab[slot_of(k)])
        lg[k] = values
        return jnp.maximum(peak, highest(values))

    peak = lax.fori_loop(0, SLOTS - 1, logits_of, jnp.full((NQ, LANES), -jnp.inf, F32))
    mx[...] = jnp.broadcast_to(jnp.max(peak, axis=1, keepdims=True), (NQ, LANES))
    sacc[...] = jnp.zeros((NQ, LANES), F32)
    positive = jnp.zeros((NQ, LANES), F32)
    for c in range(TILES):
        cols = slice(c * LANES, (c + 1) * LANES)
        positive = positive + qm[:, cols].astype(F32) * gcnt[:, cols]
    pacc[...] = positive

    def weights(k, level_ref):
        def rows(b):
            at = pl.ds(b * CHUNK, CHUNK)
            low_at = pl.ds(NQ + b * CHUNK, CHUNK)
            level = level_ref[at, :]
            s = sacc[at, :]
            for c in range(TILES):
                cols = slice(c * LANES, (c + 1) * LANES)
                e = jnp.exp(lg[k, at, cols] - level)
                s = s + e
                high = e.astype(BF16)
                coef[k, at, cols] = high
                coef[k, low_at, cols] = (e - high.astype(F32)).astype(BF16)
            sacc[at, :] = s

        each(0, nblocks, rows)

    each(0, SLOTS - 1, lambda k: weights(k, mx))

    def gradients(k):
        gacc[...] += dot(coef[k], lab[slot_of(k)])


    free_copy.wait()
    wait_all(recv.at[pl.ds(0, NCLS - 1)], d_s, d_r)
    arrived = recv[...].reshape(2 * NCLS, 3 * HALF)
    stacked = jnp.concatenate([arrived[:, r * HALF : (r + 1) * HALF] for r in range(3)], axis=0)
    swaps = []
    for h in range(2):
        at = slice(h * (ROWS // 2), (h + 1) * (ROWS // 2))
        for c in range(2):
            cols = slice(c * HALF, (c + 1) * HALF)
            fresh[core, at, cols] = (free[at, cols].astype(F32) + dot(put[c, at, :], stacked)).astype(BF16)
        swap = pltpu.make_async_remote_copy(
            fresh.at[core, at], fresh.at[core, at], f_s.at[h], f_r.at[h],
            device_id={"core": 1 - core}, device_id_type=MESH,
        )
        swap.start()
        swaps.append(swap)
    out_copy = pltpu.make_async_copy(fresh.at[core], fresh_hbm, out_sem)
    out_copy.start()
    own_logits = dot_t(qm[...], fresh[core])
    gacc[...] = dot(coef[0], lab[slot_of(0)])
    for h, swap in enumerate(swaps):
        swap.wait_recv()
        sent.append((fresh.at[0, pl.ds(0, ROWS // 2)], f_s.at[h]))
    other_logits = dot_t(qm[...], fresh[1 - core])
    peak = jnp.maximum(highest(own_logits), highest(other_logits))
    lg[SLOTS - 1, :, 0:ROWS] = jnp.where(core == 0, own_logits, other_logits)
    lg[SLOTS - 1, :, ROWS : 2 * ROWS] = jnp.where(core == 0, other_logits, own_logits)
    old = mx[...]
    top = jnp.maximum(old, jnp.broadcast_to(jnp.max(peak, axis=1, keepdims=True), (NQ, LANES)))
    sacc[...] = sacc[...] * jnp.exp(old - top)
    top_ref[...] = top
    weights(SLOTS - 1, top_ref)
    positive = pacc[...]
    for c in range(TILES):
        cols = slice(c * LANES, (c + 1) * LANES)
        positive = positive + cnt[SLOTS - 1, :, cols].astype(F32) * lg[SLOTS - 1, :, cols]
    pacc[...] = positive

    st_p[plane, 0:1, :] = top_ref[...].T[0:1, :]
    st_p[plane, 1:2, :] = jnp.sum(sacc[...].T, axis=0, keepdims=True)
    st_p[plane, 2:3, :] = jnp.sum((pacc[...] * inv[...]).T, axis=0, keepdims=True)
    st_p[plane, 3:4, :] = jnp.zeros((1, NQ), F32)

    def stats_plane(k):
        tx, ty = plane_peer(k)
        pltpu.make_async_remote_copy(
            st_p.at[plane], st_p.at[plane], sp_s, sp_r, device_id={"x": tx, "y": ty}, device_id_type=MESH
        ).start()

    each(1, NPLANE, stats_plane)
    each(1, MIDDLE, gradients)
    wait_all(st_p.at[pl.ds(0, NPLANE - 1)], sp_s, sp_r)
    peak, total, positive = merged(st_p, NPLANE)
    st_z[z, 0:1, :] = peak
    st_z[z, 1:2, :] = total
    st_z[z, 2:3, :] = positive
    st_z[z, 3:4, :] = jnp.zeros((1, NQ), F32)

    def stats_z(k):
        pltpu.make_async_remote_copy(
            st_z.at[z], st_z.at[z], sz_s, sz_r, device_id={"z": z_peer(k)}, device_id_type=MESH
        ).start()

    each(1, NZ, stats_z)
    each(MIDDLE, SLOTS - 1, gradients)
    new = fresh[...].reshape(SLOT_ROWS, D)
    last = dot(coef[SLOTS - 1], new)
    last_count = dot(cnt[SLOTS - 1], new)
    factor = jnp.exp(mx[...] - top_ref[...])
    for c in range(TILES):
        cols = slice(c * LANES, (c + 1) * LANES)
        gu[:, cols] = (gacc[0:NQ, cols] + gacc[NQ : 2 * NQ, cols]) * factor + (last[0:NQ, cols] + last[NQ : 2 * NQ, cols])
        gt[:, cols] = (gcnt[:, cols] + last_count[:, cols]) * inv[...]
    wait_all(st_z.at[pl.ds(0, NZ - 1)], sz_s, sz_r)
    peak, total, positive = merged(st_z, NZ)
    log_total = peak + jnp.log(total)
    ltb[...] = jnp.exp(top_ref[...] - jnp.broadcast_to(log_total, (LANES, NQ)).T)
    for c in range(TILES):
        cols = slice(c * LANES, (c + 1) * LANES)
        gsend[:, :, cols] = (gu[:, cols] * ltb[...] - gt[:, cols]).astype(BF16).reshape(NPLANE, 2 * NZ, LANES)

    def scatter_plane(k):
        tx, ty = plane_peer(k)
        pltpu.make_async_remote_copy(
            gsend.at[tx * NY + ty], grecv.at[plane], gp_s, gp_r, device_id={"x": tx, "y": ty}, device_id_type=MESH
        ).start()

    each(1, NPLANE, scatter_plane)
    grecv[plane] = gsend[plane]
    loss = log_total - positive
    own = (plane * NZ + z) * 2
    query = lax.broadcasted_iota(I32, (1, NQ), 1)
    for i in range(2):
        loss_ref[:, i : i + 1] = jnp.sum(jnp.where(query == own + i, loss, 0.0), axis=1, keepdims=True)
    wait_all(grecv.at[pl.ds(0, NPLANE - 1)], gp_s, gp_r)
    part = grecv[0].astype(F32)
    for i in range(1, NPLANE):
        part = part + grecv[i].astype(F32)
    hsend[...] = part.reshape(NZ, 2, D)

    def scatter_z(k):
        tz = z_peer(k)
        pltpu.make_async_remote_copy(
            hsend.at[tz], hrecv.at[z], gz_s, gz_r, device_id={"z": tz}, device_id_type=MESH
        ).start()

    each(1, NZ, scatter_z)
    hrecv[z] = hsend[z]
    out_copy.wait()
    wait_all(hrecv.at[pl.ds(0, NZ - 1)], gz_s, gz_r)
    whole = hrecv[0]
    for i in range(1, NZ):
        whole = whole + hrecv[i]
    grad_ref[...] = whole.astype(BF16)
    for ref, s in sent:
        pltpu.make_async_copy(ref, ref, s).wait()


def hand_over(loss_in, grad_in, fresh_in, loss_out, grad_out, fresh_out, loss, grad, fresh, sems):
    parts = 2
    size = ROWS // parts
    moves = [(loss_in, loss, loss_out), (grad_in, grad, grad_out)]
    for i in range(parts):
        at = pl.ds(i * size, size)
        moves.append((fresh_in.at[at], fresh.at[at], fresh_out.at[at]))
    ins = [pltpu.make_async_copy(a, b, sems.at[0, i]) for i, (a, b, _) in enumerate(moves)]
    outs = [pltpu.make_async_copy(b, c, sems.at[1, i]) for i, (_, b, c) in enumerate(moves)]
    for copy in ins:
        copy.start()
    for i in range(len(moves)):
        ins[i].wait()
        outs[i].start()
    for copy in outs:
        copy.wait()


def per_device(
    queries,
    positives,
    label_vectors,
    refresh_slot,
    features,
    encoder_weight,
    encoder_gain,
    free_vectors,
    targets,
):
    vmem = pl.BlockSpec(memory_space=pltpu.VMEM)
    hbm = pl.BlockSpec(memory_space=pl.ANY)
    dma = pltpu.SemaphoreType.DMA
    results = (
        jax.ShapeDtypeStruct((1, 2), F32),
        jax.ShapeDtypeStruct((2, D), BF16),
        jax.ShapeDtypeStruct((ROWS, D), BF16),
    )
    made = pl.pallas_call(
        kernel,
        out_shape=results,
        in_specs=[hbm] * 9,
        out_specs=(vmem, vmem, hbm),
        scratch_shapes=[
            pltpu.SMEM((1,), I32),
            pltpu.VMEM((2, POS, NQ), I32),
            pltpu.VMEM((ROWS, D), BF16),
            pltpu.VMEM((D, D), BF16),
            pltpu.VMEM((TILES, LANES), F32),
            pltpu.VMEM((2 * NCLS * 3, LANES), I32),
            pltpu.VMEM((NPLANE, NZ, 2, D), BF16),
            pltpu.VMEM((NQ, D), BF16),
            pltpu.VMEM((SLOTS, SLOT_ROWS, D), BF16),
            pltpu.VMEM((ROWS, D), BF16),
            pltpu.VMEM((2 * ROWS, HALF), BF16),
            pltpu.VMEM((NCLS, 2, 3 * HALF), BF16),
            pltpu.VMEM((NCLS, 2, 3 * HALF), BF16),
            pltpu.VMEM((2, ROWS, 3 * 2 * NCLS), BF16),
            pltpu.VMEM((2, ROWS, D), BF16),
            pltpu.VMEM((POS, NQ, LANES), I32),
            pltpu.VMEM((NQ, LANES), F32),
            pltpu.VMEM((SLOTS, NQ, SLOT_ROWS), F32),
            pltpu.VMEM((SLOTS, NQ, SLOT_ROWS), BF16),
            pltpu.VMEM((NQ, LANES), F32),
            pltpu.VMEM((NQ, LANES), F32),
            pltpu.VMEM((NQ, LANES), F32),
            pltpu.VMEM((NQ, LANES), F32),
            pltpu.VMEM((NQ, LANES), F32),
            pltpu.VMEM((SLOTS, 2 * NQ, SLOT_ROWS), BF16),
            pltpu.VMEM((2 * NQ, D), F32),
            pltpu.VMEM((NQ, D), F32),
            pltpu.VMEM((NQ, D), F32),
            pltpu.VMEM((NQ, D), F32),
            pltpu.VMEM((NPLANE, 2 * NZ, D), BF16),
            pltpu.VMEM((NPLANE, 2 * NZ, D), BF16),
            pltpu.VMEM((NZ, 2, D), F32),
            pltpu.VMEM((NZ, 2, D), F32),
            pltpu.VMEM((NPLANE, 4, NQ), F32),
            pltpu.VMEM((NZ, 4, NQ), F32),
            pltpu.SemaphoreType.REGULAR,
        ]
        + [dma] * 6
        + [dma((4,))]
        + [dma] * 6
        + [dma((2,))] * 2
        + [dma] * 8,
        compiler_params=pltpu.CompilerParams(
            collective_id=0, has_side_effects=True, vmem_limit_bytes=56 * 2**20
        ),
    )(
        refresh_slot.reshape(1),
        queries.reshape(2, D),
        jnp.swapaxes(positives, 1, 2),
        label_vectors.reshape(SLOTS, SLOT_ROWS, D),
        features,
        encoder_weight,
        encoder_gain.reshape(TILES, LANES),
        free_vectors,
        targets.reshape(-1, LANES),
    )
    loss, grads, refreshed = pl.pallas_call(
        hand_over,
        out_shape=results,
        in_specs=[hbm] * 3,
        out_specs=(hbm,) * 3,
        scratch_shapes=[
            pltpu.VMEM((1, 2), F32),
            pltpu.VMEM((2, D), BF16),
            pltpu.VMEM((ROWS, D), BF16),
            dma((2, 4)),
        ],
    )(*made)
    return loss, grads.reshape(1, 2, D), refreshed


def solution(mesh):
    torus = Mesh(mesh.devices.reshape(NY, NZ, NX, mesh.shape["rep"]), CLS_REP)
    placed = (
        P("core", CLS, None),
        P(),
        P(CLS, None),
        P(),
        P(CLS_REP, None),
        P(),
        P(),
        P(CLS_REP, None),
        P(),
    )
    return jax.shard_map(
        per_device,
        mesh=torus,
        in_specs=placed,
        out_specs=(P("core", CLS), P("core", CLS, None), P(CLS_REP, None)),
        check_vma=False,
    )
```
